32 devices in a mesh: role: 4 (over z), dp: 2 (over x), tp: 4 (over y, core).
Axes of the slice: x: 2, y: 2, z: 4, core: 2. Of those that a mesh axis runs over, the one named last changes fastest.
Arguments:
- activations: bfloat16 [2048, 8192], P(('role', 'dp'), 'tp'), may hold values from -6 to 6
- cotangent: bfloat16 [2048, 14336], P(('role', 'dp'), 'tp'), may hold values from -6 to 6
- block_keep: int32 [8], P(('role', 'dp')), may hold values 0 or 1
- input_factor: float32 [64, 8192], P(('role', 'dp'), 'tp'), may hold values from -0.5 to 0.5
- input_mean: float32 [64, 8192], P(('role', 'dp'), 'tp'), may hold values from -6 to 6
- input_square: float32 [64, 8192], P(('role', 'dp'), 'tp'), may hold values from 0.5 to 4
- output_factor: float32 [64, 14336], P(('role', 'dp'), 'tp'), may hold values from -0.3125 to 0.3125
- output_mean: float32 [64, 14336], P(('role', 'dp'), 'tp'), may hold values from -6 to 6
- output_square: float32 [64, 14336], P(('role', 'dp'), 'tp'), may hold values from 0.5 to 4
- frozen_base_rows: bfloat16 [14336, 8192], P(('dp', 'tp')), may hold values from -0.0625 to 0.0625
- prompts: bfloat16 [1024, 8192], P(('role', 'dp', 'tp')), may hold values from -6 to 6
Outputs:
- updated_input: float32 [64, 8192], P(('role', 'dp'), 'tp')
- updated_output: float32 [64, 14336], P(('role', 'dp'), 'tp')
- mean_input: float32 [64, 8192], P(('role', 'dp'), 'tp')
- mean_output: float32 [64, 14336], P(('role', 'dp'), 'tp')
- square_input: float32 [64, 8192], P(('role', 'dp'), 'tp')
- square_output: float32 [64, 14336], P(('role', 'dp'), 'tp')
- merged_weight_rows: bfloat16 [14336, 8192], P(('dp', 'tp'))
- projected: bfloat16 [14336, 1024], P(('dp', 'tp'), 'role')
The draws below stay inside these ranges and needn't reach their ends.
All inputs are finite; a program needn't handle non-finite values. No bound on the sum of `block_keep` on one device may be relied on, other than what follows from the above.
Results may differ from the reference program's by a relative error of at most 0.006.
Values may be sent and summed in bfloat16 or wider, within the bound.
A program may use at most 128 MiB of HBM per device.

```python
import math
import jax
import jax.numpy as jnp
from jax import lax

D = 8192
FFW = 14336
RANK = 64
ROLLOUT_TOKENS = 256
TOKENS = 2048
BLOCKS = 8
PROMPTS = 1024


def touch_ends(result, key, low, high):
    dims = result.shape
    place = [jax.random.randint(jax.random.fold_in(key, axis), (), 0, dims[axis]) for axis in range(len(dims))]
    result = result.at[tuple(place)].set(low)
    longest = dims.index(max(dims))
    place[longest] = (place[longest] + 1) % dims[longest]
    return result.at[tuple(place)].set(high)


def shard_levels(own_key, shape, cuts, smallest, top_value):
    factor_of, own = 1.0, jax.random.fold_in(own_key, 6)
    for dim, shards_of in cuts:
        draws = jnp.exp(jax.random.uniform(jax.random.fold_in(own, dim), (shards_of,), jnp.float32, smallest / len(cuts), top_value / len(cuts)))
        factor_of = factor_of * jnp.repeat(draws, shape[dim] // shards_of).reshape([-1 if axis == dim else 1 for axis in range(len(shape))])
    return factor_of


def scatter_about(own_key, shape, spread, limit, shards=(), dtype=jnp.bfloat16):
    array = jax.random.normal(own_key, shape, jnp.float32) * spread
    if len(shards) > 0:
        array = shard_levels(own_key, shape, shards, -0.22, 0.18) * array
    return jnp.clip(array, min=-limit, max=limit).astype(dtype)


def setup_inputs(seed: int = 0) -> dict:
    key_of = jax.random.split(jax.random.key(seed), 12)
    return {
        "activations": scatter_about(key_of[0], (TOKENS, D), 1.0, 6.0, ((0, 8), (1, 4))),
        "cotangent": scatter_about(key_of[1], (TOKENS, FFW), 1.0, 6.0, ((0, 8), (1, 4))),
        "block_keep": touch_ends((jax.random.randint(key_of[2], (BLOCKS,), 0, 4) < 3).astype(jnp.int32), jax.random.fold_in(key_of[2], 1), 0, 1),
        "input_factor": scatter_about(key_of[3], (RANK, D), 0.035, 0.5, ((0, 8), (1, 4)), jnp.float32),
        "input_mean": scatter_about(key_of[4], (RANK, D), 1.0, 6.0, ((0, 8), (1, 4)), jnp.float32),
        "input_square": jnp.clip(jnp.exp(math.log(4.0) - 2.0794415 * jax.random.uniform(key_of[5], (RANK, D), jnp.float32) ** shard_levels(key_of[5], (RANK, D), ((0, 8), (1, 4)), -0.2, 0.2)), 0.5, 4.0),
        "output_factor": scatter_about(key_of[6], (RANK, FFW), 0.02, 0.3125, ((0, 8), (1, 4)), jnp.float32),
        "output_mean": scatter_about(key_of[7], (RANK, FFW), 1.0, 6.0, ((0, 8), (1, 4)), jnp.float32),
        "output_square": jnp.clip(jnp.exp(math.log(4.0) - 2.0794415 * jax.random.uniform(key_of[8], (RANK, FFW), jnp.float32) ** shard_levels(key_of[8], (RANK, FFW), ((0, 8), (1, 4)), -0.2, 0.2)), 0.5, 4.0),
        "frozen_base_rows": scatter_about(key_of[9], (FFW, D), D ** -0.5, 0.0625, ((0, 8),)),
        "prompts": scatter_about(key_of[10], (PROMPTS, D), 1.0, 6.0, ((0, 32),)),
    }


adapter_scale = 2.0
learn_rate = 0.004
beta_one = 0.9
beta_two = 0.95
epsilon = 1e-08
first_fix = 1.0 - 0.9 ** 20
second_fix = 1.0 - 0.95 ** 20

def adam_update(factor, moment, square, gradient):
    moment_new = beta_one * moment + (1.0 - beta_one) * gradient
    square_new = beta_two * square + (1.0 - beta_two) * gradient * gradient
    factor_new = factor - learn_rate * (moment_new / first_fix) / (jnp.sqrt(square_new / second_fix) + epsilon)
    return (factor_new, moment_new, square_new)

def masked(values, block_keep):
    blocks = block_keep.shape[0]
    reshaped_rows = values.reshape(blocks, values.shape[0] // blocks, values.shape[1])
    weighted = reshaped_rows * block_keep.astype(jnp.float32)[:, None, None]
    return weighted.reshape(values.shape).astype(jnp.bfloat16)

def contract_rows(left, right):
    return lax.dot_general(left, right, (((0,), (0,)), ((), ())), preferred_element_type=jnp.float32)

def contract_cols(left, right):
    return lax.dot_general(left, right, (((1,), (1,)), ((), ())), preferred_element_type=jnp.float32)

def reference(activations, cotangent, block_keep, input_factor, input_mean, input_square, output_factor, output_mean, output_square, frozen_base_rows, prompts):
    input_rows = input_factor.astype(jnp.bfloat16)
    output_rows = output_factor.astype(jnp.bfloat16)
    low_input = jnp.dot(activations, input_rows.T, preferred_element_type=jnp.float32)
    low_grad = jnp.dot(cotangent, output_rows.T, preferred_element_type=jnp.float32)
    input_kept = masked(low_input, block_keep)
    grad_kept = masked(low_grad, block_keep)
    adapter_factor_scale = adapter_scale / ROLLOUT_TOKENS
    input_grad = contract_rows(grad_kept, activations) * adapter_factor_scale
    output_grad = contract_rows(input_kept, cotangent) * adapter_factor_scale
    input_new, input_moment, input_second = adam_update(input_factor, input_mean, input_square, input_grad)
    output_new, output_moment, output_second = adam_update(output_factor, output_mean, output_square, output_grad)
    adapter_delta_rows = contract_rows(output_new.astype(jnp.bfloat16), input_new.astype(jnp.bfloat16))
    merged_weight_rows = (frozen_base_rows.astype(jnp.float32) + adapter_scale * adapter_delta_rows).astype(jnp.bfloat16)
    projected = contract_cols(merged_weight_rows, prompts).astype(jnp.bfloat16)
    return (input_new, output_new, input_moment, output_moment, input_second, output_second, merged_weight_rows, projected)
```

```python
import functools

import jax
import jax.numpy as jnp
from jax import lax
from jax.experimental import pallas as pl
from jax.experimental.pallas import tpu as pltpu
from jax.sharding import PartitionSpec as P

ROLLOUT_TOKENS = 256


adapter_scale = 2.0
learn_rate = 0.004
beta_one = 0.9
beta_two = 0.95
epsilon = 1e-08
first_fix = 1.0 - 0.9**20
second_fix = 1.0 - 0.95**20


def adam_update(factor, moment, square, gradient):
    moment_new = beta_one * moment + (1.0 - beta_one) * gradient
    square_new = beta_two * square + (1.0 - beta_two) * gradient * gradient
    factor_new = factor - learn_rate * (moment_new / first_fix) / (
        jnp.sqrt(square_new / second_fix) + epsilon
    )
    return (factor_new, moment_new, square_new)


def masked(values, block_keep):
    blocks = block_keep.shape[0]
    reshaped_rows = values.reshape(blocks, values.shape[0] // blocks, values.shape[1])
    weighted = reshaped_rows * block_keep.astype(jnp.float32)[:, None, None]
    return weighted.reshape(values.shape).astype(jnp.bfloat16)


def contract_rows(left, right):
    return lax.dot_general(
        left, right, (((0,), (0,)), ((), ())), preferred_element_type=jnp.float32
    )


def contract_cols(left, right):
    return lax.dot_general(
        left, right, (((1,), (1,)), ((), ())), preferred_element_type=jnp.float32
    )


VMEM = pl.BlockSpec(memory_space=pltpu.VMEM)
MESH = pl.DeviceIdType.MESH


def places():
    return tuple(lax.axis_index(name) for name in ("role", "dp", "tp"))


def sizes():
    return tuple(lax.axis_size(name) for name in ("role", "dp", "tp"))


def enter(peers):
    barrier = pltpu.get_barrier_semaphore()
    for peer in peers:
        pl.semaphore_signal(barrier, inc=1, device_id=peer, device_id_type=MESH)
    pl.semaphore_wait(barrier, len(peers))


def send(source, target, send_sem, recv_sem, peer):
    copy = pltpu.make_async_remote_copy(
        src_ref=source,
        dst_ref=target,
        send_sem=send_sem,
        recv_sem=recv_sem,
        device_id=peer,
        device_id_type=MESH,
    )
    copy.start()
    return copy


def landed(slot, sem):
    pltpu.make_async_copy(slot, slot, sem).wait()


def communicate(kernel, name, outs, scratch, collective_id, args):
    return pl.pallas_call(
        kernel,
        name=name,
        out_shape=outs,
        in_specs=[VMEM] * len(args),
        out_specs=[VMEM] * len(outs),
        scratch_shapes=scratch,
        compiler_params=pltpu.CompilerParams(
            collective_id=collective_id,
            has_side_effects=True,
            vmem_limit_bytes=40 * 1024 * 1024,
        ),
        cost_estimate=pl.CostEstimate(
            flops=10**9, bytes_accessed=10**7, transcendentals=0
        ),
    )(*args)


def dma(*shape):
    return pltpu.SemaphoreType.DMA(shape)


def gather_kernel(count, *refs):
    ins, outs = refs[:count], refs[count : 2 * count]
    own, send_role, recv_role, send_dp, recv_dp = refs[2 * count :]
    role, dp, tp = places()
    roles, dps, _ = sizes()
    role_peers = [(lax.rem(role + k, roles), dp, tp) for k in range(1, roles)]
    dp_peers = [(role, lax.rem(dp + j, dps), tp) for j in range(1, dps)]
    enter(role_peers + dp_peers)
    copies = []
    for i in range(count):
        for k in range(1, roles):
            copies.append(send(ins[i], outs[i].at[dp, role], send_role.at[i, k], recv_role.at[i, k], role_peers[k - 1]))
        for j in range(1, dps):
            copies.append(send(ins[i], outs[i].at[dp, role], send_dp.at[i, j, 0], recv_dp.at[i, j, 0], dp_peers[j - 1]))
        local = pltpu.make_async_copy(ins[i], outs[i].at[dp, role], own.at[i])
        local.start()
    for i in range(count):
        for k in range(1, roles):
            slot = outs[i].at[dp, lax.rem(role + roles - k, roles)]
            landed(slot, recv_role.at[i, k])
            for j in range(1, dps):
                copies.append(send(slot, slot, send_dp.at[i, j, k], recv_dp.at[i, j, k], dp_peers[j - 1]))
    for i in range(count):
        pltpu.make_async_copy(ins[i], outs[i].at[dp, role], own.at[i]).wait()
        for j in range(1, dps):
            for k in range(roles):
                slot = outs[i].at[lax.rem(dp + dps - j, dps), lax.rem(role + roles - k, roles)]
                landed(slot, recv_dp.at[i, j, k])
    for copy in copies:
        copy.wait_send()


def gather_rows(arrays):
    roles, dps, _ = sizes()
    n = len(arrays)
    return communicate(
        functools.partial(gather_kernel, n),
        "gather_rows",
        [jax.ShapeDtypeStruct((dps, roles, *x.shape), x.dtype) for x in arrays],
        [dma(n), dma(n, roles), dma(n, roles), dma(n, dps, roles), dma(n, dps, roles)],
        0,
        arrays,
    )


def features_kernel(count, *refs):
    ins, outs = refs[:count], refs[count : 2 * count]
    slots = refs[2 * count : 3 * count]
    sends, recvs = refs[3 * count :]
    role, dp, tp = places()
    tps = sizes()[2]
    peers = [(role, dp, lax.rem(tp + k, tps)) for k in range(1, tps)]
    enter(peers)
    copies = []
    for i in range(count):
        for k in range(1, tps):
            copies.append(send(ins[i], slots[i].at[k - 1], sends.at[i, k], recvs.at[i, k], peers[k - 1]))
    for i in range(count):
        total = ins[i][...]
        for k in range(1, tps):
            landed(slots[i].at[k - 1], recvs.at[i, k])
            total = total + slots[i][k - 1]
        outs[i][...] = total
    for copy in copies:
        copy.wait_send()


def sum_features(arrays):
    tps = sizes()[2]
    n = len(arrays)
    return communicate(
        functools.partial(features_kernel, n),
        "sum_features",
        [jax.ShapeDtypeStruct(x.shape, x.dtype) for x in arrays],
        [pltpu.VMEM((max(tps - 1, 1), *x.shape), x.dtype) for x in arrays] + [dma(n, tps), dma(n, tps)],
        1,
        arrays,
    )


def tokens_kernel(count, *refs):
    ins, outs = refs[:count], refs[count : 2 * count]
    slots = refs[2 * count : 3 * count]
    sends, recvs = refs[3 * count :]
    role, dp, tp = places()
    roles, dps, _ = sizes()
    offsets = [(j, k) for k in range(roles) for j in range(dps) if (j, k) != (0, 0)]
    offsets.sort(key=lambda o: -min(o[1], roles - o[1]))
    peers = {(j, k): (lax.rem(role + k, roles), lax.rem(dp + j, dps), tp) for j, k in offsets}
    enter(list(peers.values()))
    copies = []
    for i in range(count):
        for j, k in offsets:
            peer = peers[j, k]
            copies.append(send(ins[i].at[peer[1], peer[0]], slots[i].at[j, k], sends.at[i, j, k], recvs.at[i, j, k], peer))
    for i in range(count):
        total = ins[i][dp, role].astype(jnp.float32)
        for j, k in reversed(offsets):
            landed(slots[i].at[j, k], recvs.at[i, j, k])
            total = total + slots[i][j, k].astype(jnp.float32)
        outs[i][...] = total
    for copy in copies:
        copy.wait_send()


def sum_tokens(arrays):
    roles, dps, _ = sizes()
    n = len(arrays)
    return communicate(
        functools.partial(tokens_kernel, n),
        "sum_tokens",
        [jax.ShapeDtypeStruct(x.shape[2:], jnp.float32) for x in arrays],
        [pltpu.VMEM(x.shape, x.dtype) for x in arrays] + [dma(n, dps, roles), dma(n, dps, roles)],
        2,
        arrays,
    )


def spread_kernel(a_ref, b_ref, whole_ref, slice_ref, own, send_b, recv_b, send_role, recv_role, send_dp, recv_dp, send_hi, recv_hi, send_lo, recv_lo):
    role, dp, tp = places()
    roles, dps, tps = sizes()
    half = tps // 2
    devices = roles * dps * tps
    me = (role * dps + dp) * tps + tp

    barrier = pltpu.get_barrier_semaphore()

    @pl.loop(1, devices)
    def _(step):
        other = lax.rem(me + step, devices)
        peer = (other // (dps * tps), lax.rem(other // tps, dps), lax.rem(other, tps))
        pl.semaphore_signal(barrier, inc=1, device_id=peer, device_id_type=MESH)

    pl.semaphore_wait(barrier, devices - 1)

    role_peers = [(lax.rem(role + k, roles), dp, tp) for k in range(1, roles)]
    dp_peers = [(role, lax.rem(dp + j, dps), tp) for j in range(1, dps)]
    hi_peers = [(role, dp, lax.rem(tp + 2 * h, tps)) for h in range(1, half)]
    lo_peer = (role, dp, tp + 1 - 2 * lax.rem(tp, 2))

    home = whole_ref.at[tp, dp, role]
    copies = []
    for k in range(1, roles):
        copies.append(send(a_ref, home, send_role.at[k], recv_role.at[k], role_peers[k - 1]))
    for j in range(1, dps):
        copies.append(send(a_ref, home, send_dp.at[j, 0], recv_dp.at[j, 0], dp_peers[j - 1]))
    local = pltpu.make_async_copy(a_ref, home, own.at[0])
    local.start()

    def b_copy(i, k):
        block = tp * dps + i
        peer = (lax.rem(role + k, roles), block // tps, lax.rem(block, tps))
        place = slice_ref.at[dp, role]
        remote = pltpu.make_async_remote_copy(
            src_ref=b_ref.at[i], dst_ref=place, send_sem=send_b.at[i, k], recv_sem=recv_b.at[dp, role],
            device_id=peer, device_id_type=MESH,
        )
        if k > 0:
            return None, remote, None
        here = (block // tps == dp) & (lax.rem(block, tps) == tp)
        return here, remote, pltpu.make_async_copy(b_ref.at[i], place, recv_b.at[dp, role])

    for k in range(roles):
        for i in range(dps):
            here, remote, beside = b_copy(i, k)
            if here is None:
                remote.start()
            else:
                pl.when(here)(beside.start)
                pl.when(jnp.logical_not(here))(remote.start)

    for k in range(1, roles):
        slot = whole_ref.at[tp, dp, lax.rem(role + roles - k, roles)]
        landed(slot, recv_role.at[k])
        for j in range(1, dps):
            copies.append(send(slot, slot, send_dp.at[j, k], recv_dp.at[j, k], dp_peers[j - 1]))
    local.wait()
    for j in range(dps):
        from_dp = lax.rem(dp + dps - j, dps)
        if j > 0:
            for k in range(roles):
                landed(whole_ref.at[tp, from_dp, lax.rem(role + roles - k, roles)], recv_dp.at[j, k])
        group = whole_ref.at[tp, from_dp]
        for h in range(1, half):
            copies.append(send(group, group, send_hi.at[h, j], recv_hi.at[h, j], hi_peers[h - 1]))
        copies.append(send(group, group, send_lo.at[0, j], recv_lo.at[0, j], lo_peer))
    for j in range(dps):
        from_dp = lax.rem(dp + dps - j, dps)
        for h in range(1, half):
            group = whole_ref.at[lax.rem(tp + tps - 2 * h, tps), from_dp]
            landed(group, recv_hi.at[h, j])
            copies.append(send(group, group, send_lo.at[h, j], recv_lo.at[h, j], lo_peer))
    other = lo_peer[2]
    for j in range(dps):
        from_dp = lax.rem(dp + dps - j, dps)
        for h in range(half):
            landed(whole_ref.at[lax.rem(other + tps - 2 * h, tps), from_dp], recv_lo.at[h, j])
    for d in range(dps):
        for r in range(roles):
            landed(slice_ref.at[d, r], recv_b.at[d, r])
    for k in range(roles):
        for i in range(dps):
            here, remote, _ = b_copy(i, k)
            if here is None:
                remote.wait_send()
            else:
                pl.when(jnp.logical_not(here))(remote.wait_send)
    for copy in copies:
        copy.wait_send()


def spread(a, b):
    roles, dps, tps = sizes()
    half = max(tps // 2, 1)
    return communicate(
        spread_kernel,
        "spread",
        [
            jax.ShapeDtypeStruct((tps, dps, roles, *a.shape), a.dtype),
            jax.ShapeDtypeStruct((dps, roles, *b.shape[1:]), b.dtype),
        ],
        [
            dma(1), dma(dps, roles), dma(dps, roles), dma(roles), dma(roles),
            dma(dps, roles), dma(dps, roles), dma(half, dps), dma(half, dps), dma(half, dps), dma(half, dps),
        ],
        3,
        [a, b],
    )


def merge_kernel(base_ref, b_ref, a_ref, prompts_ref, merged_ref, projected_ref):
    shards, _, width = a_ref.shape
    total = jnp.zeros(projected_ref.shape, jnp.float32)
    for shard in range(shards):
        columns = pl.ds(shard * width, width)
        delta = jnp.dot(b_ref[...], a_ref[shard], preferred_element_type=jnp.float32)
        merged = (base_ref[:, columns].astype(jnp.float32) + adapter_scale * delta).astype(jnp.bfloat16)
        merged_ref[:, columns] = merged
        total = total + contract_cols(merged, prompts_ref[:, columns])
    projected_ref[...] = total.astype(projected_ref.dtype)


def merge(base, b, a, prompts):
    rows, width = base.shape
    tile = max(t for t in range(16, 257, 16) if rows % t == 0)
    count = prompts.shape[0]
    return pl.pallas_call(
        merge_kernel,
        name="merge",
        grid=(rows // tile,),
        out_shape=[
            jax.ShapeDtypeStruct(base.shape, base.dtype),
            jax.ShapeDtypeStruct((rows, count), jnp.bfloat16),
        ],
        in_specs=[
            pl.BlockSpec((tile, width), lambda i: (i, 0)),
            pl.BlockSpec((tile, b.shape[1]), lambda i: (i, 0)),
            VMEM,
            VMEM,
        ],
        out_specs=[
            pl.BlockSpec((tile, width), lambda i: (i, 0)),
            pl.BlockSpec((tile, count), lambda i: (i, 0)),
        ],
        compiler_params=pltpu.CompilerParams(vmem_limit_bytes=56 * 1024 * 1024),
        cost_estimate=pl.CostEstimate(
            flops=2 * rows * width * (count + b.shape[1]), bytes_accessed=4 * rows * width, transcendentals=0
        ),
    )(base, b, a, prompts)


def body(
    activations,
    cotangent,
    block_keep,
    input_factor,
    input_mean,
    input_square,
    output_factor,
    output_mean,
    output_square,
    frozen_base_rows,
    prompts,
):
    roles, dps, tps = sizes()
    rows = input_factor.shape[0]
    rank = roles * dps * rows
    group_prompts = lax.all_gather(prompts, ("dp", "tp"), axis=0, tiled=True)
    input_rows, output_rows = gather_rows(
        [input_factor.astype(jnp.bfloat16), output_factor.astype(jnp.bfloat16)]
    )
    low_input = contract_cols(activations, input_rows.reshape(rank, -1))
    low_grad = contract_cols(cotangent, output_rows.reshape(rank, -1))
    low_input, low_grad = sum_features([low_input, low_grad])
    input_kept = masked(low_input, block_keep)
    grad_kept = masked(low_grad, block_keep)
    input_part = contract_rows(grad_kept, activations).astype(jnp.bfloat16)
    output_part = contract_rows(input_kept, cotangent).astype(jnp.bfloat16)
    input_sum, output_sum = sum_tokens(
        [part.reshape(dps, roles, rows, -1) for part in (input_part, output_part)]
    )
    adapter_factor_scale = adapter_scale / ROLLOUT_TOKENS
    input_new, input_moment, input_second = adam_update(
        input_factor, input_mean, input_square, input_sum * adapter_factor_scale
    )
    output_new, output_moment, output_second = adam_update(
        output_factor, output_mean, output_square, output_sum * adapter_factor_scale
    )
    input_send = input_new.astype(jnp.bfloat16)
    output_send = output_new.astype(jnp.bfloat16).reshape(rows, dps, -1).swapaxes(0, 1)
    input_whole, output_slice = spread(input_send, output_send)
    merged_weight_rows, projected = merge(
        frozen_base_rows,
        output_slice.reshape(rank, -1).T,
        input_whole.reshape(tps, rank, -1),
        group_prompts,
    )
    return (
        input_new,
        output_new,
        input_moment,
        output_moment,
        input_second,
        output_second,
        merged_weight_rows,
        projected,
    )


HBM = pl.BlockSpec(memory_space=pltpu.HBM)
SMEM = pl.BlockSpec(memory_space=pltpu.SMEM)
PARTS = 4


class Wires:
    def __init__(self, sends, recvs):
        self.sends, self.recvs, self.copies, self.used = sends, recvs, [], 0

    def send(self, source, target, peer):
        place = self.used
        self.used += 1
        self.copies.append(send(source, target, self.sends.at[place], self.recvs.at[place], peer))
        return place

    def landed(self, slot, place):
        landed(slot, self.recvs.at[place])

    def drain(self):
        for copy in self.copies:
            copy.wait_send()


def far_first(count):
    return sorted(range(1, count), key=lambda k: -min(k, count - k))


def step_kernel(
    act_hbm, cot_hbm, keep_ref, a_hbm, am_hbm, av_hbm, b_hbm, bm_hbm, bv_hbm, prompts_hbm,
    a_new, a_mom, a_sec, b_new, b_mom, b_sec, whole, piece, group,
    act, cot, a, am, av, b, bm, bv, fa, fb, la, lb, ra, rb, pa, pb, xa, xb, sa, sb, za, zb, oa, ob, b_send,
    local, sends, recvs, b_sends, b_recvs,
):
    role, dp, tp = places()
    roles, dps, tps = sizes()
    half = tps // 2
    devices = roles * dps * tps
    me = (role * dps + dp) * tps + tp
    scale = adapter_scale / ROLLOUT_TOKENS
    bf16, f32 = jnp.bfloat16, jnp.float32
    wires = Wires(sends, recvs)

    loads = {}
    pairs = [("a", a_hbm, a), ("b", b_hbm, b), ("act", act_hbm, act), ("cot", cot_hbm, cot), ("am", am_hbm, am),
             ("av", av_hbm, av), ("bm", bm_hbm, bm), ("bv", bv_hbm, bv), ("own", prompts_hbm, group.at[dp, tp])]
    for i, (name, source, target) in enumerate(pairs):
        loads[name] = pltpu.make_async_copy(source, target, local.at[i])
        loads[name].start()

    barrier = pltpu.get_barrier_semaphore()

    @pl.loop(1, devices)
    def _(step):
        other = lax.rem(me + step, devices)
        peer = (other // (dps * tps), lax.rem(other // tps, dps), lax.rem(other, tps))
        pl.semaphore_signal(barrier, inc=1, device_id=peer, device_id_type=MESH)

    loads["a"].wait()
    fa[dp, role] = a[...].astype(bf16)
    loads["b"].wait()
    fb[dp, role] = b[...].astype(bf16)
    pl.semaphore_wait(barrier, devices - 1)

    role_of = lambda k: lax.rem(role + k, roles)
    role_back = lambda k: lax.rem(role + roles - k, roles)
    dp_of = lambda j: lax.rem(dp + j, dps)
    dp_back = lambda j: lax.rem(dp + dps - j, dps)
    tp_back = lambda k: lax.rem(tp + tps - k, tps)
    role_peer = lambda k: (role_of(k), dp, tp)
    dp_peer = lambda j: (role, dp_of(j), tp)
    tp_peer = lambda k: (role, dp, lax.rem(tp + k, tps))
    other = tp + 1 - 2 * lax.rem(tp, 2)
    lo_peer = (role, dp, other)
    far = far_first(roles)
    near = far[::-1]

    def gather_start(ref):
        home = ref.at[dp, role]
        to_role = {k: wires.send(home, home, role_peer(k)) for k in near}
        to_dp = {(j, 0): wires.send(home, home, dp_peer(j)) for j in range(1, dps)}
        return to_role, to_dp

    def gather_forward(ref, to_role, to_dp):
        for k in near:
            slot = ref.at[dp, role_back(k)]
            wires.landed(slot, to_role[k])
            for j in range(1, dps):
                to_dp[j, k] = wires.send(slot, slot, dp_peer(j))

    def gather_finish(ref, to_dp):
        for (j, k), place in to_dp.items():
            wires.landed(ref.at[dp_back(j), role_back(k)], place)

    width = prompts_hbm.shape[1] // PARTS
    part = lambda ref, c: ref.at[:, pl.ds(c * width, width)]
    spot = lambda d, t, c: group.at[d, t, :, pl.ds(c * width, width)]
    via_dp = PARTS // 2
    hi_own, lo_own, dp_own, hi_far, dp_far, lo_ids = {}, {}, {}, {}, {}, {}

    def prompts_first():
        for c in range(PARTS):
            for h in range(1, half):
                hi_own[h, c] = wires.send(part(prompts_hbm, c), spot(dp, tp, c), tp_peer(2 * h))
            lo_own[c] = wires.send(part(prompts_hbm, c), spot(dp, tp, c), lo_peer)

    def prompts_across(parts):
        for c in parts:
            for j in range(1, dps):
                dp_own[j, c] = wires.send(part(prompts_hbm, c), spot(dp, tp, c), dp_peer(j))

    def prompts_hi_landed(parts):
        for c in parts:
            for h in range(1, half):
                slot = spot(dp, tp_back(2 * h), c)
                wires.landed(slot, hi_own[h, c])
                lo_ids[0, h, c] = wires.send(slot, slot, lo_peer)
                if c < via_dp:
                    for j in range(1, dps):
                        dp_far[j, h, c] = wires.send(slot, slot, dp_peer(j))

    def prompts_dp_landed(parts):
        for c in parts:
            for j in range(1, dps):
                slot = spot(dp_back(j), tp, c)
                wires.landed(slot, dp_own[j, c])
                lo_ids[j, 0, c] = wires.send(slot, slot, lo_peer)
                if c >= via_dp:
                    for h in range(1, half):
                        hi_far[j, h, c] = wires.send(slot, slot, tp_peer(2 * h))

    def prompts_far_landed():
        for c in range(PARTS):
            for j in range(1, dps):
                for h in range(1, half):
                    slot = spot(dp_back(j), tp_back(2 * h), c)
                    wires.landed(slot, dp_far[j, h, c] if c < via_dp else hi_far[j, h, c])
                    lo_ids[j, h, c] = wires.send(slot, slot, lo_peer)

    def prompts_finish():
        for c, place in lo_own.items():
            wires.landed(spot(dp, other, c), place)
        for (j, h, c), place in lo_ids.items():
            wires.landed(spot(dp_back(j), lax.rem(other + tps - 2 * h, tps), c), place)

    a_role, a_dp = gather_start(fa)
    b_role, b_dp = gather_start(fb)
    prompts_first()
    gather_forward(fa, a_role, a_dp)
    gather_forward(fb, b_role, b_dp)
    prompts_across(range(via_dp))

    def low_start(ref, to_dp, tokens, name, low):
        gather_finish(ref, to_dp)
        loads[name].wait()
        rows = ref[...].reshape(-1, ref.shape[-1])
        low[...] = contract_cols(rows, tokens[...]).astype(bf16)
        return [wires.send(low, (ra if low is la else rb).at[k - 1], tp_peer(k)) for k in range(1, tps)]

    def low_finish(low, slots, ids):
        total = low[...].astype(f32)
        for k in range(1, tps):
            wires.landed(slots.at[k - 1], ids[k - 1])
            total = total + slots[k - 1].astype(f32)
        return (total * keep_ref[0].astype(f32)).astype(bf16)

    a_low = low_start(fa, a_dp, act, "act", la)
    b_low = low_start(fb, b_dp, cot, "cot", lb)

    order = far + [0]

    def reduce_start(ref, kept, tokens, x_slots):
        grads = jnp.dot(kept, tokens[...], preferred_element_type=f32).astype(bf16)
        ref[...] = grads.reshape(ref.shape)
        ids = {}
        for k in order:
            for j in range(1, dps):
                ids[j, k] = wires.send(ref.at[dp_of(j), role_of(k)], x_slots.at[j - 1, role_of(k)], dp_peer(j))
        return ids

    def reduce_middle(ref, x_slots, x_ids, s_slots, z_slots, own):
        ids = {}
        for k in order:
            total = ref[dp, role_of(k)].astype(f32)
            for j in range(1, dps):
                wires.landed(x_slots.at[j - 1, role], x_ids[j, k]) if k == 0 else wires.landed(
                    x_slots.at[j - 1, role_of(k)], x_ids[j, k])
                total = total + x_slots[j - 1, role_of(k)].astype(f32)
            if k == 0:
                own[...] = total
            else:
                s_slots[k - 1] = total.astype(bf16)
                ids[k] = wires.send(s_slots.at[k - 1], z_slots.at[k - 1], role_peer(k))
        return ids

    def reduce_finish(own, z_slots, ids):
        total = own[...]
        for k in order[:-1]:
            wires.landed(z_slots.at[k - 1], ids[k])
            total = total + z_slots[k - 1].astype(f32)
        return total * scale

    kept_in = low_finish(la, ra, a_low)
    xb_ids = reduce_start(pb, kept_in, cot, xb)
    kept_grad = low_finish(lb, rb, b_low)
    xa_ids = reduce_start(pa, kept_grad, act, xa)
    prompts_hi_landed(range(PARTS))
    zb_ids = reduce_middle(pb, xb, xb_ids, sb, zb, ob)
    za_ids = reduce_middle(pa, xa, xa_ids, sa, za, oa)
    prompts_across(range(via_dp, PARTS))
    prompts_dp_landed(range(via_dp))

    for name in ("am", "av", "bm", "bv"):
        loads[name].wait()

    fresh, mom, sec = adam_update(b[...], bm[...], bv[...], reduce_finish(ob, zb, zb_ids))
    b_new[...], b_mom[...], b_sec[...] = fresh, mom, sec
    columns = fresh.shape[1] // dps
    for i in range(dps):
        b_send[i] = fresh[:, i * columns : (i + 1) * columns].astype(bf16)

    def b_copy(i, k):
        block = tp * dps + i
        peer = (role_of(k), block // tps, lax.rem(block, tps))
        place = piece.at[dp, role]
        remote = pltpu.make_async_remote_copy(
            src_ref=b_send.at[i], dst_ref=place, send_sem=b_sends.at[i, k], recv_sem=b_recvs.at[dp, role],
            device_id=peer, device_id_type=MESH,
        )
        if k > 0:
            return None, remote, None
        here = (block // tps == dp) & (lax.rem(block, tps) == tp)
        return here, remote, pltpu.make_async_copy(b_send.at[i], place, b_recvs.at[dp, role])

    for k in far + [0]:
        for i in range(dps):
            here, remote, beside = b_copy(i, k)
            if here is None:
                remote.start()
            else:
                pl.when(here)(beside.start)
                pl.when(jnp.logical_not(here))(remote.start)

    fresh, mom, sec = adam_update(a[...], am[...], av[...], reduce_finish(oa, za, za_ids))
    whole[tp, dp, role] = fresh.astype(bf16)
    a_new[...], a_mom[...], a_sec[...] = fresh, mom, sec
    mine = whole.at[tp]
    a_role, a_dp = gather_start(mine)
    gather_forward(mine, a_role, a_dp)
    hi_ids, lo_a = {}, {}
    for j in range(dps):
        if j > 0:
            for k in range(roles):
                wires.landed(mine.at[dp_back(j), role_back(k)], a_dp[j, k])
        slot = mine.at[dp_back(j)]
        for h in range(1, half):
            hi_ids[h, j] = wires.send(slot, slot, tp_peer(2 * h))
        lo_a[0, j] = wires.send(slot, slot, lo_peer)
    prompts_dp_landed(range(via_dp, PARTS))
    prompts_far_landed()
    for j in range(dps):
        for h in range(1, half):
            slot = whole.at[tp_back(2 * h), dp_back(j)]
            wires.landed(slot, hi_ids[h, j])
            lo_a[h, j] = wires.send(slot, slot, lo_peer)
    for (h, j), place in lo_a.items():
        wires.landed(whole.at[lax.rem(other + tps - 2 * h, tps), dp_back(j)], place)
    for d in range(dps):
        for r in range(roles):
            landed(piece.at[d, r], b_recvs.at[d, r])
    prompts_finish()
    loads["own"].wait()
    for k in range(roles):
        for i in range(dps):
            here, remote, _ = b_copy(i, k)
            if here is None:
                remote.wait_send()
            else:
                pl.when(jnp.logical_not(here))(remote.wait_send)
    wires.drain()


def step(activations, cotangent, block_keep, a, am, av, b, bm, bv, prompts):
    roles, dps, tps = sizes()
    tokens, a_width = activations.shape
    b_width = cotangent.shape[1]
    rows = a.shape[0]
    rank = roles * dps * rows
    bf16, f32 = jnp.bfloat16, jnp.float32
    vmem = pltpu.VMEM
    args = [activations, cotangent, block_keep, a, am, av, b, bm, bv, prompts]
    outs = [jax.ShapeDtypeStruct(x.shape, f32) for x in (a, a, a, b, b, b)] + [
        jax.ShapeDtypeStruct((tps, dps, roles, rows, a_width), bf16),
        jax.ShapeDtypeStruct((dps, roles, rows, b_width // dps), bf16),
        jax.ShapeDtypeStruct((dps, tps, *prompts.shape), bf16),
    ]
    wide = lambda *lead: [vmem((*lead, rows, w), bf16) for w in (a_width, b_width)]
    return pl.pallas_call(
        step_kernel,
        name="step",
        out_shape=outs,
        in_specs=[HBM, HBM, SMEM] + [HBM] * 7,
        out_specs=[VMEM] * len(outs),
        scratch_shapes=[vmem(activations.shape, bf16), vmem(cotangent.shape, bf16)]
        + [vmem(a.shape, f32)] * 3
        + [vmem(b.shape, f32)] * 3
        + wide(dps, roles)
        + [vmem((rank, tokens), bf16)] * 2
        + [vmem((tps - 1, rank, tokens), bf16)] * 2
        + wide(dps, roles)
        + wide(dps - 1, roles)
        + wide(roles - 1)
        + wide(roles - 1)
        + [vmem(a.shape, f32), vmem(b.shape, f32), vmem((dps, rows, b_width // dps), bf16)]
        + [dma(9), dma(160), dma(160), dma(dps, roles), dma(dps, roles)],
        compiler_params=pltpu.CompilerParams(
            collective_id=0, has_side_effects=True, vmem_limit_bytes=40 * 1024 * 1024
        ),
        cost_estimate=pl.CostEstimate(flops=10**9, bytes_accessed=10**7, transcendentals=0),
    )(*args)


def finish_kernel(base_ref, b_ref, a_ref, prompts_ref, *refs):
    small, (merged_ref, projected_ref), copies = refs[:6], refs[6:8], refs[8:]

    @pl.when(pl.program_id(0) == 0)
    def _():
        for source, target in zip(small, copies):
            target[...] = source[...]

    shards, _, width = a_ref.shape
    total = jnp.zeros(projected_ref.shape, jnp.float32)
    for shard in range(shards):
        columns = pl.ds(shard * width, width)
        delta = contract_rows(b_ref[...], a_ref[shard])
        merged = (base_ref[:, columns].astype(jnp.float32) + adapter_scale * delta).astype(jnp.bfloat16)
        merged_ref[:, columns] = merged
        total = total + contract_cols(merged, prompts_ref[:, columns])
    projected_ref[...] = total.astype(projected_ref.dtype)


def finish(base, b, a, prompts, small):
    rows, width = base.shape
    tile = max(t for t in range(128, 257, 128) if rows % t == 0)
    count = prompts.shape[0]
    return pl.pallas_call(
        finish_kernel,
        name="finish",
        grid=(rows // tile,),
        out_shape=[
            jax.ShapeDtypeStruct(base.shape, base.dtype),
            jax.ShapeDtypeStruct((rows, count), jnp.bfloat16),
        ]
        + [jax.ShapeDtypeStruct(x.shape, x.dtype) for x in small],
        in_specs=[
            pl.BlockSpec((tile, width), lambda i: (i, 0)),
            pl.BlockSpec((b.shape[0], tile), lambda i: (0, i)),
        ]
        + [VMEM] * (2 + len(small)),
        out_specs=[
            pl.BlockSpec((tile, width), lambda i: (i, 0)),
            pl.BlockSpec((tile, count), lambda i: (i, 0)),
        ]
        + [VMEM] * len(small),
        compiler_params=pltpu.CompilerParams(vmem_limit_bytes=40 * 1024 * 1024),
        cost_estimate=pl.CostEstimate(
            flops=2 * rows * width * (count + b.shape[0]), bytes_accessed=4 * rows * width, transcendentals=0
        ),
    )(base, b, a, prompts, *small)


def fused_body(
    activations, cotangent, block_keep, input_factor, input_mean, input_square,
    output_factor, output_mean, output_square, frozen_base_rows, prompts,
):
    roles, dps, tps = sizes()
    rank = roles * dps * input_factor.shape[0]
    *small, whole, piece, group = step(
        activations, cotangent, block_keep, input_factor, input_mean, input_square,
        output_factor, output_mean, output_square, prompts,
    )
    merged, projected, *copies = finish(
        frozen_base_rows,
        piece.reshape(rank, -1),
        whole.reshape(tps, rank, -1),
        group.reshape(-1, prompts.shape[1]),
        small,
    )
    a_new, a_mom, a_sec, b_new, b_mom, b_sec = copies
    return a_new, b_new, a_mom, b_mom, a_sec, b_sec, merged, projected


def chosen_body(*args):
    roles, dps, tps = sizes()
    blocks, rows = args[2].shape[0], args[3].shape[0]
    base_rows = args[9].shape[0]
    fits = rows % 8 == 0 and args[10].shape[0] % 8 == 0 and base_rows % 128 == 0
    if blocks == 1 and min(roles, dps) > 1 and tps % 2 == 0 and fits:
        return fused_body(*args)
    return body(*args)


def solution(mesh):
    placed = (
        P(("role", "dp"), "tp"),
        P(("role", "dp"), "tp"),
        P(("role", "dp")),
        P(("role", "dp"), "tp"),
        P(("role", "dp"), "tp"),
        P(("role", "dp"), "tp"),
        P(("role", "dp"), "tp"),
        P(("role", "dp"), "tp"),
        P(("role", "dp"), "tp"),
        P(("dp", "tp"), None),
        P(("role", "dp", "tp"), None),
    )
    return jax.shard_map(
        chosen_body,
        mesh=mesh,
        in_specs=placed,
        out_specs=(
            P(("role", "dp"), "tp"),
            P(("role", "dp"), "tp"),
            P(("role", "dp"), "tp"),
            P(("role", "dp"), "tp"),
            P(("role", "dp"), "tp"),
            P(("role", "dp"), "tp"),
            P(("dp", "tp"), None),
            P(("dp", "tp"), "role"),
        ),
        check_vma=False,
    )
```

```python
import functools

import jax
import jax.numpy as jnp
from jax import lax
from jax.experimental import pallas as pl
from jax.experimental.pallas import tpu as pltpu
from jax.sharding import PartitionSpec as P

ROLLOUT_TOKENS = 256


adapter_scale = 2.0
learn_rate = 0.004
beta_one = 0.9
beta_two = 0.95
epsilon = 1e-08
first_fix = 1.0 - 0.9**20
second_fix = 1.0 - 0.95**20


def adam_update(factor, moment, square, gradient):
    moment_new = beta_one * moment + (1.0 - beta_one) * gradient
    square_new = beta_two * square + (1.0 - beta_two) * gradient * gradient
    factor_new = factor - learn_rate * (moment_new / first_fix) / (
        jnp.sqrt(square_new / second_fix) + epsilon
    )
    return (factor_new, moment_new, square_new)


def masked(values, block_keep):
    blocks = block_keep.shape[0]
    reshaped_rows = values.reshape(blocks, values.shape[0] // blocks, values.shape[1])
    weighted = reshaped_rows * block_keep.astype(jnp.float32)[:, None, None]
    return weighted.reshape(values.shape).astype(jnp.bfloat16)


def contract_rows(left, right):
    return lax.dot_general(
        left, right, (((0,), (0,)), ((), ())), preferred_element_type=jnp.float32
    )


def contract_cols(left, right):
    return lax.dot_general(
        left, right, (((1,), (1,)), ((), ())), preferred_element_type=jnp.float32
    )


VMEM = pl.BlockSpec(memory_space=pltpu.VMEM)
MESH = pl.DeviceIdType.MESH


def places():
    return tuple(lax.axis_index(name) for name in ("role", "dp", "tp"))


def sizes():
    return tuple(lax.axis_size(name) for name in ("role", "dp", "tp"))


def enter(peers):
    barrier = pltpu.get_barrier_semaphore()
    for peer in peers:
        pl.semaphore_signal(barrier, inc=1, device_id=peer, device_id_type=MESH)
    pl.semaphore_wait(barrier, len(peers))


def send(source, target, send_sem, recv_sem, peer):
    copy = pltpu.make_async_remote_copy(
        src_ref=source,
        dst_ref=target,
        send_sem=send_sem,
        recv_sem=recv_sem,
        device_id=peer,
        device_id_type=MESH,
    )
    copy.start()
    return copy


def landed(slot, sem):
    pltpu.make_async_copy(slot, slot, sem).wait()


def communicate(kernel, name, outs, scratch, collective_id, args):
    return pl.pallas_call(
        kernel,
        name=name,
        out_shape=outs,
        in_specs=[VMEM] * len(args),
        out_specs=[VMEM] * len(outs),
        scratch_shapes=scratch,
        compiler_params=pltpu.CompilerParams(
            collective_id=collective_id,
            has_side_effects=True,
            vmem_limit_bytes=40 * 1024 * 1024,
        ),
        cost_estimate=pl.CostEstimate(
            flops=10**9, bytes_accessed=10**7, transcendentals=0
        ),
    )(*args)


def dma(*shape):
    return pltpu.SemaphoreType.DMA(shape)


def gather_kernel(count, *refs):
    ins, outs = refs[:count], refs[count : 2 * count]
    own, send_role, recv_role, send_dp, recv_dp = refs[2 * count :]
    role, dp, tp = places()
    roles, dps, _ = sizes()
    role_peers = [(lax.rem(role + k, roles), dp, tp) for k in range(1, roles)]
    dp_peers = [(role, lax.rem(dp + j, dps), tp) for j in range(1, dps)]
    enter(role_peers + dp_peers)
    copies = []
    for i in range(count):
        for k in range(1, roles):
            copies.append(send(ins[i], outs[i].at[dp, role], send_role.at[i, k], recv_role.at[i, k], role_peers[k - 1]))
        for j in range(1, dps):
            copies.append(send(ins[i], outs[i].at[dp, role], send_dp.at[i, j, 0], recv_dp.at[i, j, 0], dp_peers[j - 1]))
        local = pltpu.make_async_copy(ins[i], outs[i].at[dp, role], own.at[i])
        local.start()
    for i in range(count):
        for k in range(1, roles):
            slot = outs[i].at[dp, lax.rem(role + roles - k, roles)]
            landed(slot, recv_role.at[i, k])
            for j in range(1, dps):
                copies.append(send(slot, slot, send_dp.at[i, j, k], recv_dp.at[i, j, k], dp_peers[j - 1]))
    for i in range(count):
        pltpu.make_async_copy(ins[i], outs[i].at[dp, role], own.at[i]).wait()
        for j in range(1, dps):
            for k in range(roles):
                slot = outs[i].at[lax.rem(dp + dps - j, dps), lax.rem(role + roles - k, roles)]
                landed(slot, recv_dp.at[i, j, k])
    for copy in copies:
        copy.wait_send()


def gather_rows(arrays):
    roles, dps, _ = sizes()
    n = len(arrays)
    return communicate(
        functools.partial(gather_kernel, n),
        "gather_rows",
        [jax.ShapeDtypeStruct((dps, roles, *x.shape), x.dtype) for x in arrays],
        [dma(n), dma(n, roles), dma(n, roles), dma(n, dps, roles), dma(n, dps, roles)],
        0,
        arrays,
    )


def features_kernel(count, *refs):
    ins, outs = refs[:count], refs[count : 2 * count]
    slots = refs[2 * count : 3 * count]
    sends, recvs = refs[3 * count :]
    role, dp, tp = places()
    tps = sizes()[2]
    peers = [(role, dp, lax.rem(tp + k, tps)) for k in range(1, tps)]
    enter(peers)
    copies = []
    for i in range(count):
        for k in range(1, tps):
            copies.append(send(ins[i], slots[i].at[k - 1], sends.at[i, k], recvs.at[i, k], peers[k - 1]))
    for i in range(count):
        total = ins[i][...]
        for k in range(1, tps):
            landed(slots[i].at[k - 1], recvs.at[i, k])
            total = total + slots[i][k - 1]
        outs[i][...] = total
    for copy in copies:
        copy.wait_send()


def sum_features(arrays):
    tps = sizes()[2]
    n = len(arrays)
    return communicate(
        functools.partial(features_kernel, n),
        "sum_features",
        [jax.ShapeDtypeStruct(x.shape, x.dtype) for x in arrays],
        [pltpu.VMEM((max(tps - 1, 1), *x.shape), x.dtype) for x in arrays] + [dma(n, tps), dma(n, tps)],
        1,
        arrays,
    )


def tokens_kernel(count, *refs):
    ins, outs = refs[:count], refs[count : 2 * count]
    slots = refs[2 * count : 3 * count]
    sends, recvs = refs[3 * count :]
    role, dp, tp = places()
    roles, dps, _ = sizes()
    offsets = [(j, k) for k in range(roles) for j in range(dps) if (j, k) != (0, 0)]
    offsets.sort(key=lambda o: -min(o[1], roles - o[1]))
    peers = {(j, k): (lax.rem(role + k, roles), lax.rem(dp + j, dps), tp) for j, k in offsets}
    enter(list(peers.values()))
    copies = []
    for i in range(count):
        for j, k in offsets:
            peer = peers[j, k]
            copies.append(send(ins[i].at[peer[1], peer[0]], slots[i].at[j, k], sends.at[i, j, k], recvs.at[i, j, k], peer))
    for i in range(count):
        total = ins[i][dp, role].astype(jnp.float32)
        for j, k in reversed(offsets):
            landed(slots[i].at[j, k], recvs.at[i, j, k])
            total = total + slots[i][j, k].astype(jnp.float32)
        outs[i][...] = total
    for copy in copies:
        copy.wait_send()


def sum_tokens(arrays):
    roles, dps, _ = sizes()
    n = len(arrays)
    return communicate(
        functools.partial(tokens_kernel, n),
        "sum_tokens",
        [jax.ShapeDtypeStruct(x.shape[2:], jnp.float32) for x in arrays],
        [pltpu.VMEM(x.shape, x.dtype) for x in arrays] + [dma(n, dps, roles), dma(n, dps, roles)],
        2,
        arrays,
    )


def spread_kernel(a_ref, b_ref, whole_ref, slice_ref, own, send_b, recv_b, send_role, recv_role, send_dp, recv_dp, send_hi, recv_hi, send_lo, recv_lo):
    role, dp, tp = places()
    roles, dps, tps = sizes()
    half = tps // 2
    devices = roles * dps * tps
    me = (role * dps + dp) * tps + tp

    barrier = pltpu.get_barrier_semaphore()

    @pl.loop(1, devices)
    def _(step):
        other = lax.rem(me + step, devices)
        peer = (other // (dps * tps), lax.rem(other // tps, dps), lax.rem(other, tps))
        pl.semaphore_signal(barrier, inc=1, device_id=peer, device_id_type=MESH)

    pl.semaphore_wait(barrier, devices - 1)

    role_peers = [(lax.rem(role + k, roles), dp, tp) for k in range(1, roles)]
    dp_peers = [(role, lax.rem(dp + j, dps), tp) for j in range(1, dps)]
    hi_peers = [(role, dp, lax.rem(tp + 2 * h, tps)) for h in range(1, half)]
    lo_peer = (role, dp, tp + 1 - 2 * lax.rem(tp, 2))

    home = whole_ref.at[tp, dp, role]
    copies = []
    for k in range(1, roles):
        copies.append(send(a_ref, home, send_role.at[k], recv_role.at[k], role_peers[k - 1]))
    for j in range(1, dps):
        copies.append(send(a_ref, home, send_dp.at[j, 0], recv_dp.at[j, 0], dp_peers[j - 1]))
    local = pltpu.make_async_copy(a_ref, home, own.at[0])
    local.start()

    def b_copy(i, k):
        block = tp * dps + i
        peer = (lax.rem(role + k, roles), block // tps, lax.rem(block, tps))
        place = slice_ref.at[dp, role]
        remote = pltpu.make_async_remote_copy(
            src_ref=b_ref.at[i], dst_ref=place, send_sem=send_b.at[i, k], recv_sem=recv_b.at[dp, role],
            device_id=peer, device_id_type=MESH,
        )
        if k > 0:
            return None, remote, None
        here = (block // tps == dp) & (lax.rem(block, tps) == tp)
        return here, remote, pltpu.make_async_copy(b_ref.at[i], place, recv_b.at[dp, role])

    for k in range(roles):
        for i in range(dps):
            here, remote, beside = b_copy(i, k)
            if here is None:
                remote.start()
            else:
                pl.when(here)(beside.start)
                pl.when(jnp.logical_not(here))(remote.start)

    for k in range(1, roles):
        slot = whole_ref.at[tp, dp, lax.rem(role + roles - k, roles)]
        landed(slot, recv_role.at[k])
        for j in range(1, dps):
            copies.append(send(slot, slot, send_dp.at[j, k], recv_dp.at[j, k], dp_peers[j - 1]))
    local.wait()
    for j in range(dps):
        from_dp = lax.rem(dp + dps - j, dps)
        if j > 0:
            for k in range(roles):
                landed(whole_ref.at[tp, from_dp, lax.rem(role + roles - k, roles)], recv_dp.at[j, k])
        group = whole_ref.at[tp, from_dp]
        for h in range(1, half):
            copies.append(send(group, group, send_hi.at[h, j], recv_hi.at[h, j], hi_peers[h - 1]))
        copies.append(send(group, group, send_lo.at[0, j], recv_lo.at[0, j], lo_peer))
    for j in range(dps):
        from_dp = lax.rem(dp + dps - j, dps)
        for h in range(1, half):
            group = whole_ref.at[lax.rem(tp + tps - 2 * h, tps), from_dp]
            landed(group, recv_hi.at[h, j])
            copies.append(send(group, group, send_lo.at[h, j], recv_lo.at[h, j], lo_peer))
    other = lo_peer[2]
    for j in range(dps):
        from_dp = lax.rem(dp + dps - j, dps)
        for h in range(half):
            landed(whole_ref.at[lax.rem(other + tps - 2 * h, tps), from_dp], recv_lo.at[h, j])
    for d in range(dps):
        for r in range(roles):
            landed(slice_ref.at[d, r], recv_b.at[d, r])
    for k in range(roles):
        for i in range(dps):
            here, remote, _ = b_copy(i, k)
            if here is None:
                remote.wait_send()
            else:
                pl.when(jnp.logical_not(here))(remote.wait_send)
    for copy in copies:
        copy.wait_send()


def spread(a, b):
    roles, dps, tps = sizes()
    half = max(tps // 2, 1)
    return communicate(
        spread_kernel,
        "spread",
        [
            jax.ShapeDtypeStruct((tps, dps, roles, *a.shape), a.dtype),
            jax.ShapeDtypeStruct((dps, roles, *b.shape[1:]), b.dtype),
        ],
        [
            dma(1), dma(dps, roles), dma(dps, roles), dma(roles), dma(roles),
            dma(dps, roles), dma(dps, roles), dma(half, dps), dma(half, dps), dma(half, dps), dma(half, dps),
        ],
        3,
        [a, b],
    )


def merge_kernel(base_ref, b_ref, a_ref, prompts_ref, merged_ref, projected_ref):
    shards, _, width = a_ref.shape
    total = jnp.zeros(projected_ref.shape, jnp.float32)
    for shard in range(shards):
        columns = pl.ds(shard * width, width)
        delta = jnp.dot(b_ref[...], a_ref[shard], preferred_element_type=jnp.float32)
        merged = (base_ref[:, columns].astype(jnp.float32) + adapter_scale * delta).astype(jnp.bfloat16)
        merged_ref[:, columns] = merged
        total = total + contract_cols(merged, prompts_ref[:, columns])
    projected_ref[...] = total.astype(projected_ref.dtype)


def merge(base, b, a, prompts):
    rows, width = base.shape
    tile = max(t for t in range(16, 257, 16) if rows % t == 0)
    count = prompts.shape[0]
    return pl.pallas_call(
        merge_kernel,
        name="merge",
        grid=(rows // tile,),
        out_shape=[
            jax.ShapeDtypeStruct(base.shape, base.dtype),
            jax.ShapeDtypeStruct((rows, count), jnp.bfloat16),
        ],
        in_specs=[
            pl.BlockSpec((tile, width), lambda i: (i, 0)),
            pl.BlockSpec((tile, b.shape[1]), lambda i: (i, 0)),
            VMEM,
            VMEM,
        ],
        out_specs=[
            pl.BlockSpec((tile, width), lambda i: (i, 0)),
            pl.BlockSpec((tile, count), lambda i: (i, 0)),
        ],
        compiler_params=pltpu.CompilerParams(vmem_limit_bytes=56 * 1024 * 1024),
        cost_estimate=pl.CostEstimate(
            flops=2 * rows * width * (count + b.shape[1]), bytes_accessed=4 * rows * width, transcendentals=0
        ),
    )(base, b, a, prompts)


def body(
    activations,
    cotangent,
    block_keep,
    input_factor,
    input_mean,
    input_square,
    output_factor,
    output_mean,
    output_square,
    frozen_base_rows,
    prompts,
):
    roles, dps, tps = sizes()
    rows = input_factor.shape[0]
    rank = roles * dps * rows
    group_prompts = lax.all_gather(prompts, ("dp", "tp"), axis=0, tiled=True)
    input_rows, output_rows = gather_rows(
        [input_factor.astype(jnp.bfloat16), output_factor.astype(jnp.bfloat16)]
    )
    low_input = contract_cols(activations, input_rows.reshape(rank, -1))
    low_grad = contract_cols(cotangent, output_rows.reshape(rank, -1))
    low_input, low_grad = sum_features([low_input, low_grad])
    input_kept = masked(low_input, block_keep)
    grad_kept = masked(low_grad, block_keep)
    input_part = contract_rows(grad_kept, activations).astype(jnp.bfloat16)
    output_part = contract_rows(input_kept, cotangent).astype(jnp.bfloat16)
    input_sum, output_sum = sum_tokens(
        [part.reshape(dps, roles, rows, -1) for part in (input_part, output_part)]
    )
    adapter_factor_scale = adapter_scale / ROLLOUT_TOKENS
    input_new, input_moment, input_second = adam_update(
        input_factor, input_mean, input_square, input_sum * adapter_factor_scale
    )
    output_new, output_moment, output_second = adam_update(
        output_factor, output_mean, output_square, output_sum * adapter_factor_scale
    )
    input_send = input_new.astype(jnp.bfloat16)
    output_send = output_new.astype(jnp.bfloat16).reshape(rows, dps, -1).swapaxes(0, 1)
    input_whole, output_slice = spread(input_send, output_send)
    merged_weight_rows, projected = merge(
        frozen_base_rows,
        output_slice.reshape(rank, -1).T,
        input_whole.reshape(tps, rank, -1),
        group_prompts,
    )
    return (
        input_new,
        output_new,
        input_moment,
        output_moment,
        input_second,
        output_second,
        merged_weight_rows,
        projected,
    )


HBM = pl.BlockSpec(memory_space=pltpu.HBM)
SMEM = pl.BlockSpec(memory_space=pltpu.SMEM)
PARTS = 8
ACROSS = 0


class Wires:
    def __init__(self, sends, recvs):
        self.sends, self.recvs, self.copies, self.used = sends, recvs, [], 0

    def send(self, source, target, peer):
        place = self.used
        self.used += 1
        self.copies.append(send(source, target, self.sends.at[place], self.recvs.at[place], peer))
        return place

    def landed(self, slot, place):
        landed(slot, self.recvs.at[place])

    def drain(self):
        for copy in self.copies:
            copy.wait_send()


def far_first(count):
    return sorted(range(1, count), key=lambda k: -min(k, count - k))


def step_kernel(
    act_hbm, cot_hbm, keep_ref, a_hbm, am_hbm, av_hbm, b_hbm, bm_hbm, bv_hbm, prompts_hbm, base_hbm,
    a_new, a_mom, a_sec, b_new, b_mom, b_sec, whole, piece, group, base, product,
    act, cot, a, am, av, b, bm, bv, fa, fb, la, lb, ra, rb, pa, pb, xa, xb, sa, sb, za, zb, oa, ob, b_send,
    local, sends, recvs, b_sends, b_recvs,
):
    role, dp, tp = places()
    roles, dps, tps = sizes()
    half = tps // 2
    devices = roles * dps * tps
    me = (role * dps + dp) * tps + tp
    scale = adapter_scale / ROLLOUT_TOKENS
    bf16, f32 = jnp.bfloat16, jnp.float32
    wires = Wires(sends, recvs)

    loads = {}
    pairs = [("a", a_hbm, a), ("b", b_hbm, b), ("act", act_hbm, act), ("cot", cot_hbm, cot), ("am", am_hbm, am),
             ("av", av_hbm, av), ("bm", bm_hbm, bm), ("bv", bv_hbm, bv), ("own", prompts_hbm, group.at[dp, tp])]
    for i, (name, source, target) in enumerate(pairs):
        loads[name] = pltpu.make_async_copy(source, target, local.at[i])
        loads[name].start()
    loads["base"] = pltpu.make_async_copy(base_hbm, base, local.at[len(pairs)])

    barrier = pltpu.get_barrier_semaphore()

    @pl.loop(1, devices)
    def _(step):
        other = lax.rem(me + step, devices)
        peer = (other // (dps * tps), lax.rem(other // tps, dps), lax.rem(other, tps))
        pl.semaphore_signal(barrier, inc=1, device_id=peer, device_id_type=MESH)

    loads["a"].wait()
    fa[dp, role] = a[...].astype(bf16)
    loads["b"].wait()
    fb[dp, role] = b[...].astype(bf16)
    pl.semaphore_wait(barrier, devices - 1)

    role_of = lambda k: lax.rem(role + k, roles)
    role_back = lambda k: lax.rem(role + roles - k, roles)
    dp_of = lambda j: lax.rem(dp + j, dps)
    dp_back = lambda j: lax.rem(dp + dps - j, dps)
    tp_back = lambda k: lax.rem(tp + tps - k, tps)
    role_peer = lambda k: (role_of(k), dp, tp)
    dp_peer = lambda j: (role, dp_of(j), tp)
    tp_peer = lambda k: (role, dp, lax.rem(tp + k, tps))
    other = tp + 1 - 2 * lax.rem(tp, 2)
    lo_peer = (role, dp, other)
    far = far_first(roles)
    near = far[::-1]

    def gather_start(ref):
        home = ref.at[dp, role]
        to_role = {k: wires.send(home, home, role_peer(k)) for k in near}
        to_dp = {(j, 0): wires.send(home, home, dp_peer(j)) for j in range(1, dps)}
        return to_role, to_dp

    def gather_forward(ref, to_role, to_dp, steps):
        for k in steps:
            slot = ref.at[dp, role_back(k)]
            wires.landed(slot, to_role[k])
            for j in range(1, dps):
                to_dp[j, k] = wires.send(slot, slot, dp_peer(j))

    def gather_finish(ref, to_dp):
        for (j, k), place in to_dp.items():
            wires.landed(ref.at[dp_back(j), role_back(k)], place)

    width = prompts_hbm.shape[1] // PARTS
    part = lambda ref, c: ref.at[:, pl.ds(c * width, width)]
    spot = lambda d, t, c: group.at[d, t, :, pl.ds(c * width, width)]
    hi_own, lo_own, dp_own, far_ids, lo_ids = {}, {}, {}, {}, {}

    def prompts_near(parts):
        for c in parts:
            for h in range(1, half):
                hi_own[h, c] = wires.send(part(prompts_hbm, c), spot(dp, tp, c), tp_peer(2 * h))
            lo_own[c] = wires.send(part(prompts_hbm, c), spot(dp, tp, c), lo_peer)

    def prompts_across(parts):
        for c in parts:
            for j in range(1, dps):
                dp_own[j, c] = wires.send(part(prompts_hbm, c), spot(dp, tp, c), dp_peer(j))

    def prompts_hi_landed(parts):
        for c in parts:
            for h in range(1, half):
                slot = spot(dp, tp_back(2 * h), c)
                wires.landed(slot, hi_own[h, c])
                lo_ids[0, h, c] = wires.send(slot, slot, lo_peer)
                if c >= PARTS - ACROSS:
                    for j in range(1, dps):
                        far_ids[j, h, c] = wires.send(slot, slot, dp_peer(j))

    def prompts_dp_landed(parts):
        for c in parts:
            for j in range(1, dps):
                slot = spot(dp_back(j), tp, c)
                wires.landed(slot, dp_own[j, c])
                lo_ids[j, 0, c] = wires.send(slot, slot, lo_peer)
                if c < PARTS - ACROSS:
                    for h in range(1, half):
                        far_ids[j, h, c] = wires.send(slot, slot, tp_peer(2 * h))

    def prompts_far_landed(parts):
        for c in parts:
            for j in range(1, dps):
                for h in range(1, half):
                    slot = spot(dp_back(j), tp_back(2 * h), c)
                    wires.landed(slot, far_ids[j, h, c])
                    lo_ids[j, h, c] = wires.send(slot, slot, lo_peer)

    def prompts_finish(parts):
        for c in parts:
            wires.landed(spot(dp, other, c), lo_own[c])
            for j in range(dps):
                for h in range(half):
                    if (j, h) != (0, 0):
                        wires.landed(spot(dp_back(j), lax.rem(other + tps - 2 * h, tps), c), lo_ids[j, h, c])

    def multiply(parts):
        columns = pl.ds(parts[0] * width, len(parts) * width)
        right = group[:, :, :, columns].reshape(-1, len(parts) * width)
        tiles = 4
        tile = product.shape[0] // tiles

        @pl.loop(0, tiles)
        def _(i):
            rows = pl.ds(pl.multiple_of(i * tile, tile), tile)
            term = contract_cols(base[rows, columns], right)
            product[rows, :] = term if parts[0] == 0 else product[rows, :] + term

    def low_start(ref, to_dp, tokens, name, low, slots):
        gather_finish(ref, to_dp)
        loads[name].wait()
        rows = ref[...].reshape(-1, ref.shape[-1])
        low[...] = contract_cols(rows, tokens[...]).astype(bf16)
        return [wires.send(low, slots.at[k - 1], tp_peer(k)) for k in range(1, tps)]

    def low_finish(low, slots, ids):
        total = low[...].astype(f32)
        for k in range(1, tps):
            wires.landed(slots.at[k - 1], ids[k - 1])
            total = total + slots[k - 1].astype(f32)
        return (total * keep_ref[0].astype(f32)).astype(bf16)

    order = far + [0]

    def reduce_start(ref, kept, tokens, x_slots):
        grads = jnp.dot(kept, tokens[...], preferred_element_type=f32).astype(bf16)
        ref[...] = grads.reshape(ref.shape)
        ids = {}
        for k in order:
            for j in range(1, dps):
                ids[j, k] = wires.send(ref.at[dp_of(j), role_of(k)], x_slots.at[j - 1, role_of(k)], dp_peer(j))
        return ids

    def reduce_middle(ref, x_slots, x_ids, s_slots, z_slots, own, steps):
        ids = {}
        for k in steps:
            total = ref[dp, role_of(k)].astype(f32)
            for j in range(1, dps):
                wires.landed(x_slots.at[j - 1, role_of(k)], x_ids[j, k])
                total = total + x_slots[j - 1, role_of(k)].astype(f32)
            if k == 0:
                own[...] = total
            else:
                s_slots[k - 1] = total.astype(bf16)
                ids[k] = wires.send(s_slots.at[k - 1], z_slots.at[k - 1], role_peer(k))
        return ids

    def reduce_finish(own, z_slots, ids):
        total = own[...]
        for k in near:
            wires.landed(z_slots.at[k - 1], ids[k])
            total = total + z_slots[k - 1].astype(f32)
        return total * scale

    def b_copy(i, k):
        block = tp * dps + i
        peer = (role_of(k), block // tps, lax.rem(block, tps))
        place = piece.at[dp, role]
        remote = pltpu.make_async_remote_copy(
            src_ref=b_send.at[i], dst_ref=place, send_sem=b_sends.at[i, k], recv_sem=b_recvs.at[dp, role],
            device_id=peer, device_id_type=MESH,
        )
        if k > 0:
            return None, remote, None
        here = (block // tps == dp) & (lax.rem(block, tps) == tp)
        return here, remote, pltpu.make_async_copy(b_send.at[i], place, b_recvs.at[dp, role])

    def b_start():
        for k in order:
            for i in range(dps):
                here, remote, beside = b_copy(i, k)
                if here is None:
                    remote.start()
                else:
                    pl.when(here)(beside.start)
                    pl.when(jnp.logical_not(here))(remote.start)

    def b_finish():
        for d in range(dps):
            for r in range(roles):
                landed(piece.at[d, r], b_recvs.at[d, r])
        for k in range(roles):
            for i in range(dps):
                here, remote, _ = b_copy(i, k)
                if here is None:
                    remote.wait_send()
                else:
                    pl.when(jnp.logical_not(here))(remote.wait_send)

    first, second, third, fourth = [range(i * PARTS // 4, (i + 1) * PARTS // 4) for i in range(4)]

    b_role, b_dp = gather_start(fb)
    a_role, a_dp = gather_start(fa)
    prompts_near(range(PARTS))
    prompts_across(first)
    gather_forward(fb, b_role, b_dp, near)
    loads["base"].start()
    gather_forward(fa, a_role, a_dp, near[:-1])
    b_low = low_start(fb, b_dp, cot, "cot", lb, rb)
    gather_forward(fa, a_role, a_dp, near[-1:])
    prompts_across(second)
    a_low = low_start(fa, a_dp, act, "act", la, ra)

    kept_grad = low_finish(lb, rb, b_low)
    xa_ids = reduce_start(pa, kept_grad, act, xa)
    kept_in = low_finish(la, ra, a_low)
    xb_ids = reduce_start(pb, kept_in, cot, xb)
    prompts_across(third)
    prompts_dp_landed(first)
    za_ids = reduce_middle(pa, xa, xa_ids, sa, za, oa, order)
    prompts_hi_landed(range(PARTS))
    zb_ids = reduce_middle(pb, xb, xb_ids, sb, zb, ob, order[:2])
    prompts_dp_landed(second)

    for name in ("am", "av", "bm", "bv"):
        loads[name].wait()
    fresh, mom, sec = adam_update(a[...], am[...], av[...], reduce_finish(oa, za, za_ids))
    whole[tp, dp, role] = fresh.astype(bf16)
    a_new[...], a_mom[...], a_sec[...] = fresh, mom, sec

    mine = whole.at[tp]
    hi_ids, lo_a = {}, {}

    def onward(j, k):
        slot = mine.at[dp_back(j), role_back(k)]
        for h in range(1, half):
            hi_ids[h, j, k] = wires.send(slot, slot, tp_peer(2 * h))
        lo_a[0, j, k] = wires.send(slot, slot, lo_peer)

    a_role, a_dp = gather_start(mine)
    onward(0, 0)
    zb_ids.update(reduce_middle(pb, xb, xb_ids, sb, zb, ob, order[2:]))
    for k in near:
        gather_forward(mine, a_role, a_dp, [k])
        onward(0, k)
    prompts_across(fourth)

    fresh, mom, sec = adam_update(b[...], bm[...], bv[...], reduce_finish(ob, zb, zb_ids))
    b_new[...], b_mom[...], b_sec[...] = fresh, mom, sec
    columns = fresh.shape[1] // dps
    for i in range(dps):
        b_send[i] = fresh[:, i * columns : (i + 1) * columns].astype(bf16)
    b_start()
    for j in range(1, dps):
        for k in [0] + near:
            wires.landed(mine.at[dp_back(j), role_back(k)], a_dp[j, k])
            onward(j, k)
    prompts_dp_landed(third)
    loads["own"].wait()
    loads["base"].wait()
    prompts_far_landed(first)
    prompts_far_landed(second)
    prompts_finish(first)
    prompts_finish(second)
    multiply([*first, *second])
    prompts_dp_landed(fourth)
    for j in range(dps):
        for k in [0] + near:
            for h in range(1, half):
                slot = whole.at[tp_back(2 * h), dp_back(j), role_back(k)]
                wires.landed(slot, hi_ids[h, j, k])
                lo_a[h, j, k] = wires.send(slot, slot, lo_peer)
    prompts_far_landed(third)
    prompts_far_landed(fourth)
    prompts_finish(third)
    prompts_finish(fourth)
    multiply([*third, *fourth])
    for (h, j, k), place in lo_a.items():
        wires.landed(whole.at[lax.rem(other + tps - 2 * h, tps), dp_back(j), role_back(k)], place)
    b_finish()
    wires.drain()


def step(activations, cotangent, block_keep, a, am, av, b, bm, bv, prompts, base):
    roles, dps, tps = sizes()
    tokens, a_width = activations.shape
    b_width = cotangent.shape[1]
    rows = a.shape[0]
    rank = roles * dps * rows
    bf16, f32 = jnp.bfloat16, jnp.float32
    vmem = pltpu.VMEM
    args = [activations, cotangent, block_keep, a, am, av, b, bm, bv, prompts, base]
    args = [x if x is block_keep else pltpu.with_memory_space_constraint(x, pltpu.HBM) for x in args]
    outs = [vmem(x.shape, f32) for x in (a, a, a, b, b, b)] + [
        vmem((tps, dps, roles, rows, a_width), bf16),
        vmem((dps, roles, rows, b_width // dps), bf16),
        vmem((dps, tps, *prompts.shape), bf16),
        vmem(base.shape, bf16),
        vmem((base.shape[0], dps * tps * prompts.shape[0]), f32),
    ]
    wide = lambda *lead: [vmem((*lead, rows, w), bf16) for w in (a_width, b_width)]
    return pl.pallas_call(
        step_kernel,
        name="step",
        out_shape=outs,
        in_specs=[HBM, HBM, SMEM] + [HBM] * 8,
        out_specs=[VMEM] * len(outs),
        scratch_shapes=[vmem(activations.shape, bf16), vmem(cotangent.shape, bf16)]
        + [vmem(a.shape, f32)] * 3
        + [vmem(b.shape, f32)] * 3
        + wide(dps, roles)
        + [vmem((rank, tokens), bf16)] * 2
        + [vmem((tps - 1, rank, tokens), bf16)] * 2
        + wide(dps, roles)
        + wide(dps - 1, roles)
        + wide(roles - 1)
        + wide(roles - 1)
        + [vmem(a.shape, f32), vmem(b.shape, f32), vmem((dps, rows, b_width // dps), bf16)]
        + [dma(10), dma(240), dma(240), dma(dps, roles), dma(dps, roles)],
        compiler_params=pltpu.CompilerParams(
            collective_id=0, has_side_effects=True, vmem_limit_bytes=16 * 1024 * 1024
        ),
        cost_estimate=pl.CostEstimate(flops=10**9, bytes_accessed=10**7, transcendentals=0),
    )(*args)


def finish_kernel(*refs):
    small, (base, b, a, prompts, product) = refs[:6], refs[6:11]
    copies, (merged_hbm, projected_hbm) = refs[11:17], refs[17:19]
    stage, projected, sems, out_sems, small_sems = refs[19:]
    saves = [pltpu.make_async_copy(x, y, small_sems.at[i]) for i, (x, y) in enumerate(zip(small, copies))]
    for save in saves:
        save.start()
    depth, shards, tile, width = stage.shape
    tiles = base.shape[0] // tile

    def out(i, shard):
        rows = pl.ds(pl.multiple_of(i * tile, tile), tile)
        slot = lax.rem(i, depth)
        target = merged_hbm.at[rows, shard * width : (shard + 1) * width]
        return pltpu.make_async_copy(stage.at[slot, shard], target, sems.at[slot, shard])

    @pl.loop(0, tiles)
    def _(i):
        rows = pl.ds(pl.multiple_of(i * tile, tile), tile)
        left = b[:, rows] * adapter_scale
        for shard in range(shards):

            @pl.when(i >= depth)
            def _():
                out(i - depth, shard).wait()

        for shard in range(shards):
            delta = contract_rows(left, a[shard])
            merged = base[rows, shard * width : (shard + 1) * width].astype(jnp.float32) + delta
            stage[lax.rem(i, depth), shard] = merged.astype(stage.dtype)
            out(i, shard).start()

    low = jnp.zeros((a.shape[1], prompts.shape[0]), jnp.float32)
    for shard in range(shards):
        low = low + contract_cols(a[shard], prompts[:, shard * width : (shard + 1) * width])
    high = low.astype(jnp.bfloat16)
    rest = (low - high.astype(jnp.float32)).astype(jnp.bfloat16)

    saved = []
    for i in range(base.shape[0] // tile):
        rows = pl.ds(i * tile, tile)
        extra = contract_rows(b[:, rows], high) + contract_rows(b[:, rows], rest)
        projected[rows, :] = (product[rows, :] + adapter_scale * extra).astype(projected.dtype)
    last = pltpu.make_async_copy(projected, projected_hbm, out_sems.at[0])
    last.start()

    for i in range(max(tiles - depth, 0), tiles):
        for shard in range(shards):
            out(i, shard).wait()

    for save in saves + [last]:
        save.wait()


def finish(base, b, a, prompts, product, small):
    rows, width = base.shape
    tile = max(t for t in range(128, 257, 128) if rows % t == 0)
    count = prompts.shape[0]
    shards, _, part = a.shape
    vmem = pltpu.VMEM
    args = [pltpu.with_memory_space_constraint(x, pltpu.VMEM) for x in (*small, base, b, a, prompts, product)]
    return pl.pallas_call(
        finish_kernel,
        name="finish",
        out_shape=[pltpu.HBM(x.shape, x.dtype) for x in (*small, base)]
        + [pltpu.HBM((rows, count), jnp.bfloat16)],
        in_specs=[VMEM] * len(args),
        out_specs=[HBM] * (len(small) + 2),
        scratch_shapes=[vmem((2, shards, tile, part), base.dtype), vmem((rows, count), jnp.bfloat16), dma(2, shards), dma(1), dma(len(small))],
        compiler_params=pltpu.CompilerParams(vmem_limit_bytes=16 * 1024 * 1024),
        cost_estimate=pl.CostEstimate(
            flops=2 * rows * width * (count + b.shape[0]), bytes_accessed=4 * rows * width, transcendentals=0
        ),
    )(*args)


def fused_body(
    activations, cotangent, block_keep, input_factor, input_mean, input_square,
    output_factor, output_mean, output_square, frozen_base_rows, prompts,
):
    roles, dps, tps = sizes()
    rank = roles * dps * input_factor.shape[0]
    *small, whole, piece, group, base, product = step(
        activations, cotangent, block_keep, input_factor, input_mean, input_square,
        output_factor, output_mean, output_square, prompts, frozen_base_rows,
    )
    *copies, merged, projected = finish(
        base,
        piece.reshape(rank, -1),
        whole.reshape(tps, rank, -1),
        group.reshape(-1, prompts.shape[1]),
        product,
        small,
    )
    a_new, a_mom, a_sec, b_new, b_mom, b_sec = copies
    return a_new, b_new, a_mom, b_mom, a_sec, b_sec, merged, projected


def chosen_body(*args):
    roles, dps, tps = sizes()
    blocks, rows = args[2].shape[0], args[3].shape[0]
    base_rows = args[9].shape[0]
    fits = rows % 8 == 0 and args[10].shape[0] % 8 == 0 and base_rows % 128 == 0
    if blocks == 1 and min(roles, dps) > 1 and tps % 2 == 0 and fits:
        return fused_body(*args)
    return body(*args)


def solution(mesh):
    placed = (
        P(("role", "dp"), "tp"),
        P(("role", "dp"), "tp"),
        P(("role", "dp")),
        P(("role", "dp"), "tp"),
        P(("role", "dp"), "tp"),
        P(("role", "dp"), "tp"),
        P(("role", "dp"), "tp"),
        P(("role", "dp"), "tp"),
        P(("role", "dp"), "tp"),
        P(("dp", "tp"), None),
        P(("role", "dp", "tp"), None),
    )
    return jax.shard_map(
        chosen_body,
        mesh=mesh,
        in_specs=placed,
        out_specs=(
            P(("role", "dp"), "tp"),
            P(("role", "dp"), "tp"),
            P(("role", "dp"), "tp"),
            P(("role", "dp"), "tp"),
            P(("role", "dp"), "tp"),
            P(("role", "dp"), "tp"),
            P(("dp", "tp"), None),
            P(("dp", "tp"), "role"),
        ),
        check_vma=False,
    )
```

```python
import functools
import math

import jax
import jax.numpy as jnp
from jax import lax
from jax.experimental import pallas as pl
from jax.experimental.pallas import tpu as pltpu
from jax.sharding import PartitionSpec as P

ROLLOUT_TOKENS = 256


adapter_scale = 2.0
learn_rate = 0.004
beta_one = 0.9
beta_two = 0.95
epsilon = 1e-08
first_fix = 1.0 - 0.9**20
second_fix = 1.0 - 0.95**20


def adam_update(factor, moment, square, gradient):
    moment_new = beta_one * moment + (1.0 - beta_one) * gradient
    square_new = beta_two * square + (1.0 - beta_two) * gradient * gradient
    factor_new = factor - learn_rate * (moment_new / first_fix) / (
        jnp.sqrt(square_new / second_fix) + epsilon
    )
    return (factor_new, moment_new, square_new)


def masked(values, block_keep):
    blocks = block_keep.shape[0]
    reshaped_rows = values.reshape(blocks, values.shape[0] // blocks, values.shape[1])
    weighted = reshaped_rows * block_keep.astype(jnp.float32)[:, None, None]
    return weighted.reshape(values.shape).astype(jnp.bfloat16)


def contract_rows(left, right):
    return lax.dot_general(
        left, right, (((0,), (0,)), ((), ())), preferred_element_type=jnp.float32
    )


def contract_cols(left, right):
    return lax.dot_general(
        left, right, (((1,), (1,)), ((), ())), preferred_element_type=jnp.float32
    )


VMEM = pl.BlockSpec(memory_space=pltpu.VMEM)
MESH = pl.DeviceIdType.MESH


def places():
    return tuple(lax.axis_index(name) for name in ("role", "dp", "tp"))


def sizes():
    return tuple(lax.axis_size(name) for name in ("role", "dp", "tp"))


def enter(peers):
    barrier = pltpu.get_barrier_semaphore()
    for peer in peers:
        pl.semaphore_signal(barrier, inc=1, device_id=peer, device_id_type=MESH)
    pl.semaphore_wait(barrier, len(peers))


def send(source, target, send_sem, recv_sem, peer):
    copy = pltpu.make_async_remote_copy(
        src_ref=source,
        dst_ref=target,
        send_sem=send_sem,
        recv_sem=recv_sem,
        device_id=peer,
        device_id_type=MESH,
    )
    copy.start()
    return copy


def landed(slot, sem):
    pltpu.make_async_copy(slot, slot, sem).wait()


def communicate(kernel, name, outs, scratch, collective_id, args):
    return pl.pallas_call(
        kernel,
        name=name,
        out_shape=outs,
        in_specs=[VMEM] * len(args),
        out_specs=[VMEM] * len(outs),
        scratch_shapes=scratch,
        compiler_params=pltpu.CompilerParams(
            collective_id=collective_id,
            has_side_effects=True,
            vmem_limit_bytes=40 * 1024 * 1024,
        ),
        cost_estimate=pl.CostEstimate(
            flops=10**9, bytes_accessed=10**7, transcendentals=0
        ),
    )(*args)


def dma(*shape):
    return pltpu.SemaphoreType.DMA(shape)


def gather_kernel(count, *refs):
    ins, outs = refs[:count], refs[count : 2 * count]
    own, send_role, recv_role, send_dp, recv_dp = refs[2 * count :]
    role, dp, tp = places()
    roles, dps, _ = sizes()
    role_peers = [(lax.rem(role + k, roles), dp, tp) for k in range(1, roles)]
    dp_peers = [(role, lax.rem(dp + j, dps), tp) for j in range(1, dps)]
    enter(role_peers + dp_peers)
    copies = []
    for i in range(count):
        for k in range(1, roles):
            copies.append(send(ins[i], outs[i].at[dp, role], send_role.at[i, k], recv_role.at[i, k], role_peers[k - 1]))
        for j in range(1, dps):
            copies.append(send(ins[i], outs[i].at[dp, role], send_dp.at[i, j, 0], recv_dp.at[i, j, 0], dp_peers[j - 1]))
        local = pltpu.make_async_copy(ins[i], outs[i].at[dp, role], own.at[i])
        local.start()
    for i in range(count):
        for k in range(1, roles):
            slot = outs[i].at[dp, lax.rem(role + roles - k, roles)]
            landed(slot, recv_role.at[i, k])
            for j in range(1, dps):
                copies.append(send(slot, slot, send_dp.at[i, j, k], recv_dp.at[i, j, k], dp_peers[j - 1]))
    for i in range(count):
        pltpu.make_async_copy(ins[i], outs[i].at[dp, role], own.at[i]).wait()
        for j in range(1, dps):
            for k in range(roles):
                slot = outs[i].at[lax.rem(dp + dps - j, dps), lax.rem(role + roles - k, roles)]
                landed(slot, recv_dp.at[i, j, k])
    for copy in copies:
        copy.wait_send()


def gather_rows(arrays):
    roles, dps, _ = sizes()
    n = len(arrays)
    return communicate(
        functools.partial(gather_kernel, n),
        "gather_rows",
        [jax.ShapeDtypeStruct((dps, roles, *x.shape), x.dtype) for x in arrays],
        [dma(n), dma(n, roles), dma(n, roles), dma(n, dps, roles), dma(n, dps, roles)],
        0,
        arrays,
    )


def features_kernel(count, *refs):
    ins, outs = refs[:count], refs[count : 2 * count]
    slots = refs[2 * count : 3 * count]
    sends, recvs = refs[3 * count :]
    role, dp, tp = places()
    tps = sizes()[2]
    peers = [(role, dp, lax.rem(tp + k, tps)) for k in range(1, tps)]
    enter(peers)
    copies = []
    for i in range(count):
        for k in range(1, tps):
            copies.append(send(ins[i], slots[i].at[k - 1], sends.at[i, k], recvs.at[i, k], peers[k - 1]))
    for i in range(count):
        total = ins[i][...]
        for k in range(1, tps):
            landed(slots[i].at[k - 1], recvs.at[i, k])
            total = total + slots[i][k - 1]
        outs[i][...] = total
    for copy in copies:
        copy.wait_send()


def sum_features(arrays):
    tps = sizes()[2]
    n = len(arrays)
    return communicate(
        functools.partial(features_kernel, n),
        "sum_features",
        [jax.ShapeDtypeStruct(x.shape, x.dtype) for x in arrays],
        [pltpu.VMEM((max(tps - 1, 1), *x.shape), x.dtype) for x in arrays] + [dma(n, tps), dma(n, tps)],
        1,
        arrays,
    )


def tokens_kernel(count, *refs):
    ins, outs = refs[:count], refs[count : 2 * count]
    slots = refs[2 * count : 3 * count]
    sends, recvs = refs[3 * count :]
    role, dp, tp = places()
    roles, dps, _ = sizes()
    offsets = [(j, k) for k in range(roles) for j in range(dps) if (j, k) != (0, 0)]
    offsets.sort(key=lambda o: -min(o[1], roles - o[1]))
    peers = {(j, k): (lax.rem(role + k, roles), lax.rem(dp + j, dps), tp) for j, k in offsets}
    enter(list(peers.values()))
    copies = []
    for i in range(count):
        for j, k in offsets:
            peer = peers[j, k]
            copies.append(send(ins[i].at[peer[1], peer[0]], slots[i].at[j, k], sends.at[i, j, k], recvs.at[i, j, k], peer))
    for i in range(count):
        total = ins[i][dp, role].astype(jnp.float32)
        for j, k in reversed(offsets):
            landed(slots[i].at[j, k], recvs.at[i, j, k])
            total = total + slots[i][j, k].astype(jnp.float32)
        outs[i][...] = total
    for copy in copies:
        copy.wait_send()


def sum_tokens(arrays):
    roles, dps, _ = sizes()
    n = len(arrays)
    return communicate(
        functools.partial(tokens_kernel, n),
        "sum_tokens",
        [jax.ShapeDtypeStruct(x.shape[2:], jnp.float32) for x in arrays],
        [pltpu.VMEM(x.shape, x.dtype) for x in arrays] + [dma(n, dps, roles), dma(n, dps, roles)],
        2,
        arrays,
    )


def spread_kernel(a_ref, b_ref, whole_ref, slice_ref, own, send_b, recv_b, send_role, recv_role, send_dp, recv_dp, send_hi, recv_hi, send_lo, recv_lo):
    role, dp, tp = places()
    roles, dps, tps = sizes()
    half = tps // 2
    devices = roles * dps * tps
    me = (role * dps + dp) * tps + tp

    barrier = pltpu.get_barrier_semaphore()

    @pl.loop(1, devices)
    def _(step):
        other = lax.rem(me + step, devices)
        peer = (other // (dps * tps), lax.rem(other // tps, dps), lax.rem(other, tps))
        pl.semaphore_signal(barrier, inc=1, device_id=peer, device_id_type=MESH)

    pl.semaphore_wait(barrier, devices - 1)

    role_peers = [(lax.rem(role + k, roles), dp, tp) for k in range(1, roles)]
    dp_peers = [(role, lax.rem(dp + j, dps), tp) for j in range(1, dps)]
    hi_peers = [(role, dp, lax.rem(tp + 2 * h, tps)) for h in range(1, half)]
    lo_peer = (role, dp, tp + 1 - 2 * lax.rem(tp, 2))

    home = whole_ref.at[tp, dp, role]
    copies = []
    for k in range(1, roles):
        copies.append(send(a_ref, home, send_role.at[k], recv_role.at[k], role_peers[k - 1]))
    for j in range(1, dps):
        copies.append(send(a_ref, home, send_dp.at[j, 0], recv_dp.at[j, 0], dp_peers[j - 1]))
    local = pltpu.make_async_copy(a_ref, home, own.at[0])
    local.start()

    def b_copy(i, k):
        block = tp * dps + i
        peer = (lax.rem(role + k, roles), block // tps, lax.rem(block, tps))
        place = slice_ref.at[dp, role]
        remote = pltpu.make_async_remote_copy(
            src_ref=b_ref.at[i], dst_ref=place, send_sem=send_b.at[i, k], recv_sem=recv_b.at[dp, role],
            device_id=peer, device_id_type=MESH,
        )
        if k > 0:
            return None, remote, None
        here = (block // tps == dp) & (lax.rem(block, tps) == tp)
        return here, remote, pltpu.make_async_copy(b_ref.at[i], place, recv_b.at[dp, role])

    for k in range(roles):
        for i in range(dps):
            here, remote, beside = b_copy(i, k)
            if here is None:
                remote.start()
            else:
                pl.when(here)(beside.start)
                pl.when(jnp.logical_not(here))(remote.start)

    for k in range(1, roles):
        slot = whole_ref.at[tp, dp, lax.rem(role + roles - k, roles)]
        landed(slot, recv_role.at[k])
        for j in range(1, dps):
            copies.append(send(slot, slot, send_dp.at[j, k], recv_dp.at[j, k], dp_peers[j - 1]))
    local.wait()
    for j in range(dps):
        from_dp = lax.rem(dp + dps - j, dps)
        if j > 0:
            for k in range(roles):
                landed(whole_ref.at[tp, from_dp, lax.rem(role + roles - k, roles)], recv_dp.at[j, k])
        group = whole_ref.at[tp, from_dp]
        for h in range(1, half):
            copies.append(send(group, group, send_hi.at[h, j], recv_hi.at[h, j], hi_peers[h - 1]))
        copies.append(send(group, group, send_lo.at[0, j], recv_lo.at[0, j], lo_peer))
    for j in range(dps):
        from_dp = lax.rem(dp + dps - j, dps)
        for h in range(1, half):
            group = whole_ref.at[lax.rem(tp + tps - 2 * h, tps), from_dp]
            landed(group, recv_hi.at[h, j])
            copies.append(send(group, group, send_lo.at[h, j], recv_lo.at[h, j], lo_peer))
    other = lo_peer[2]
    for j in range(dps):
        from_dp = lax.rem(dp + dps - j, dps)
        for h in range(half):
            landed(whole_ref.at[lax.rem(other + tps - 2 * h, tps), from_dp], recv_lo.at[h, j])
    for d in range(dps):
        for r in range(roles):
            landed(slice_ref.at[d, r], recv_b.at[d, r])
    for k in range(roles):
        for i in range(dps):
            here, remote, _ = b_copy(i, k)
            if here is None:
                remote.wait_send()
            else:
                pl.when(jnp.logical_not(here))(remote.wait_send)
    for copy in copies:
        copy.wait_send()


def spread(a, b):
    roles, dps, tps = sizes()
    half = max(tps // 2, 1)
    return communicate(
        spread_kernel,
        "spread",
        [
            jax.ShapeDtypeStruct((tps, dps, roles, *a.shape), a.dtype),
            jax.ShapeDtypeStruct((dps, roles, *b.shape[1:]), b.dtype),
        ],
        [
            dma(1), dma(dps, roles), dma(dps, roles), dma(roles), dma(roles),
            dma(dps, roles), dma(dps, roles), dma(half, dps), dma(half, dps), dma(half, dps), dma(half, dps),
        ],
        3,
        [a, b],
    )


def merge_kernel(base_ref, b_ref, a_ref, prompts_ref, merged_ref, projected_ref):
    shards, _, width = a_ref.shape
    total = jnp.zeros(projected_ref.shape, jnp.float32)
    for shard in range(shards):
        columns = pl.ds(shard * width, width)
        delta = jnp.dot(b_ref[...], a_ref[shard], preferred_element_type=jnp.float32)
        merged = (base_ref[:, columns].astype(jnp.float32) + adapter_scale * delta).astype(jnp.bfloat16)
        merged_ref[:, columns] = merged
        total = total + contract_cols(merged, prompts_ref[:, columns])
    projected_ref[...] = total.astype(projected_ref.dtype)


def merge(base, b, a, prompts):
    rows, width = base.shape
    tile = max(t for t in range(16, 257, 16) if rows % t == 0)
    count = prompts.shape[0]
    return pl.pallas_call(
        merge_kernel,
        name="merge",
        grid=(rows // tile,),
        out_shape=[
            jax.ShapeDtypeStruct(base.shape, base.dtype),
            jax.ShapeDtypeStruct((rows, count), jnp.bfloat16),
        ],
        in_specs=[
            pl.BlockSpec((tile, width), lambda i: (i, 0)),
            pl.BlockSpec((tile, b.shape[1]), lambda i: (i, 0)),
            VMEM,
            VMEM,
        ],
        out_specs=[
            pl.BlockSpec((tile, width), lambda i: (i, 0)),
            pl.BlockSpec((tile, count), lambda i: (i, 0)),
        ],
        compiler_params=pltpu.CompilerParams(vmem_limit_bytes=56 * 1024 * 1024),
        cost_estimate=pl.CostEstimate(
            flops=2 * rows * width * (count + b.shape[1]), bytes_accessed=4 * rows * width, transcendentals=0
        ),
    )(base, b, a, prompts)


def body(
    activations,
    cotangent,
    block_keep,
    input_factor,
    input_mean,
    input_square,
    output_factor,
    output_mean,
    output_square,
    frozen_base_rows,
    prompts,
):
    roles, dps, tps = sizes()
    rows = input_factor.shape[0]
    rank = roles * dps * rows
    group_prompts = lax.all_gather(prompts, ("dp", "tp"), axis=0, tiled=True)
    input_rows, output_rows = gather_rows(
        [input_factor.astype(jnp.bfloat16), output_factor.astype(jnp.bfloat16)]
    )
    low_input = contract_cols(activations, input_rows.reshape(rank, -1))
    low_grad = contract_cols(cotangent, output_rows.reshape(rank, -1))
    low_input, low_grad = sum_features([low_input, low_grad])
    input_kept = masked(low_input, block_keep)
    grad_kept = masked(low_grad, block_keep)
    input_part = contract_rows(grad_kept, activations).astype(jnp.bfloat16)
    output_part = contract_rows(input_kept, cotangent).astype(jnp.bfloat16)
    input_sum, output_sum = sum_tokens(
        [part.reshape(dps, roles, rows, -1) for part in (input_part, output_part)]
    )
    adapter_factor_scale = adapter_scale / ROLLOUT_TOKENS
    input_new, input_moment, input_second = adam_update(
        input_factor, input_mean, input_square, input_sum * adapter_factor_scale
    )
    output_new, output_moment, output_second = adam_update(
        output_factor, output_mean, output_square, output_sum * adapter_factor_scale
    )
    input_send = input_new.astype(jnp.bfloat16)
    output_send = output_new.astype(jnp.bfloat16).reshape(rows, dps, -1).swapaxes(0, 1)
    input_whole, output_slice = spread(input_send, output_send)
    merged_weight_rows, projected = merge(
        frozen_base_rows,
        output_slice.reshape(rank, -1).T,
        input_whole.reshape(tps, rank, -1),
        group_prompts,
    )
    return (
        input_new,
        output_new,
        input_moment,
        output_moment,
        input_second,
        output_second,
        merged_weight_rows,
        projected,
    )


HBM = pl.BlockSpec(memory_space=pltpu.HBM)
SMEM = pl.BlockSpec(memory_space=pltpu.SMEM)
PARTS = 4
ARRIVALS = 66


class Wires:
    def __init__(self, sends, recvs, ruler):
        self.sends, self.recvs, self.ruler, self.used, self.sent = sends, recvs, ruler, 0, 0

    def take(self):
        self.used += 1
        return self.used - 1

    def send(self, source, target, peer, place=None):
        place = self.take() if place is None else place
        send(source, target, self.sends.at[0], self.recvs.at[place], peer)
        self.sent += math.prod(source.shape) * source.dtype.itemsize
        return place

    def landed(self, slot, place):
        landed(slot, self.recvs.at[place])

    def drain(self):
        rows, width = self.ruler.shape
        tiles, rest = divmod(self.sent, 8 * 128 * self.ruler.dtype.itemsize)
        wide = max(w for w in range(1, width // 128 + 1) if tiles % w == 0)
        assert rest == 0 and tiles // wide * 8 <= rows
        landed(self.ruler.at[pl.ds(0, tiles // wide * 8), pl.ds(0, wide * 128)], self.sends.at[0])


def far_first(count):
    return sorted(range(1, count), key=lambda k: -min(k, count - k))


def step_kernel(
    act_hbm, cot_hbm, keep_ref, a_hbm, am_hbm, av_hbm, b_hbm, bm_hbm, bv_hbm, prompts_hbm, base_hbm,
    a_new, a_mom, a_sec, b_new, b_mom, b_sec, whole, piece, group, base, product,
    act, cot, a, am, av, b, bm, bv, fa, fb, la, lb, ra, rb, pa, pb, xa, xb, sa, sb, za, zb, oa, ob, b_send,
    local, sends, recvs, b_sends, b_recvs,
):
    role, dp, tp = places()
    roles, dps, tps = sizes()
    half = tps // 2
    devices = roles * dps * tps
    me = (role * dps + dp) * tps + tp
    scale = adapter_scale / ROLLOUT_TOKENS
    bf16, f32 = jnp.bfloat16, jnp.float32
    wires = Wires(sends, recvs, base_hbm)

    loads = {}
    pairs = [("a", a_hbm, a), ("b", b_hbm, b), ("act", act_hbm, act), ("cot", cot_hbm, cot), ("am", am_hbm, am),
             ("av", av_hbm, av), ("bm", bm_hbm, bm), ("bv", bv_hbm, bv), ("own", prompts_hbm, group.at[dp, tp])]
    for i, (name, source, target) in enumerate(pairs):
        loads[name] = pltpu.make_async_copy(source, target, local.at[i])
        loads[name].start()
    loads["base"] = pltpu.make_async_copy(base_hbm, base, local.at[len(pairs)])

    barrier = pltpu.get_barrier_semaphore()

    @pl.loop(1, devices)
    def _(step):
        other = lax.rem(me + step, devices)
        peer = (other // (dps * tps), lax.rem(other // tps, dps), lax.rem(other, tps))
        pl.semaphore_signal(barrier, inc=1, device_id=peer, device_id_type=MESH)

    loads["a"].wait()
    fa[dp, role] = a[...].astype(bf16)
    loads["b"].wait()
    fb[dp, role] = b[...].astype(bf16)
    pl.semaphore_wait(barrier, devices - 1)

    role_of = lambda k: lax.rem(role + k, roles)
    role_back = lambda k: lax.rem(role + roles - k, roles)
    dp_of = lambda j: lax.rem(dp + j, dps)
    dp_back = lambda j: lax.rem(dp + dps - j, dps)
    tp_back = lambda k: lax.rem(tp + tps - k, tps)
    role_peer = lambda k: (role_of(k), dp, tp)
    dp_peer = lambda j: (role, dp_of(j), tp)
    tp_peer = lambda k: (role, dp, lax.rem(tp + k, tps))
    other = tp + 1 - 2 * lax.rem(tp, 2)
    lo_peer = (role, dp, other)
    far = far_first(roles)
    near = far[::-1]

    def gather_start(ref):
        home = ref.at[dp, role]
        to_role = {k: wires.send(home, home, role_peer(k)) for k in near}
        to_dp = {(j, 0): wires.send(home, home, dp_peer(j)) for j in range(1, dps)}
        return to_role, to_dp

    def gather_forward(ref, to_role, to_dp, steps):
        for k in steps:
            slot = ref.at[dp, role_back(k)]
            wires.landed(slot, to_role[k])
            for j in range(1, dps):
                to_dp[j, k] = wires.send(slot, slot, dp_peer(j))

    def gather_finish(ref, to_dp):
        for (j, k), place in to_dp.items():
            wires.landed(ref.at[dp_back(j), role_back(k)], place)

    width = prompts_hbm.shape[1] // PARTS
    part = lambda ref, c: ref.at[:, pl.ds(c * width, width)]
    spot = lambda d, t, c: group.at[d, t, :, pl.ds(c * width, width)]
    hi_own, dp_own, far_ids = {}, {}, {}
    shared = [wires.take() for _ in range(PARTS)]

    def prompts_near(parts):
        for c in parts:
            for h in range(1, half):
                hi_own[h, c] = wires.send(part(prompts_hbm, c), spot(dp, tp, c), tp_peer(2 * h))
            wires.send(part(prompts_hbm, c), spot(dp, tp, c), lo_peer, shared[c])

    def prompts_across(parts):
        for c in parts:
            for j in range(1, dps):
                dp_own[j, c] = wires.send(part(prompts_hbm, c), spot(dp, tp, c), dp_peer(j))

    def prompts_hi_landed(parts):
        for c in parts:
            for h in range(1, half):
                slot = spot(dp, tp_back(2 * h), c)
                wires.landed(slot, hi_own[h, c])
                wires.send(slot, slot, lo_peer, shared[c])

    def prompts_dp_landed(parts):
        for c in parts:
            for j in range(1, dps):
                slot = spot(dp_back(j), tp, c)
                wires.landed(slot, dp_own[j, c])
                wires.send(slot, slot, lo_peer, shared[c])
                for h in range(1, half):
                    far_ids[j, h, c] = wires.send(slot, slot, tp_peer(2 * h))

    def prompts_far_landed(parts):
        for c in parts:
            for j in range(1, dps):
                for h in range(1, half):
                    slot = spot(dp_back(j), tp_back(2 * h), c)
                    wires.landed(slot, far_ids[j, h, c])
                    wires.send(slot, slot, lo_peer, shared[c])

    def prompts_finish(c):
        wires.landed(group.at[:, pl.ds(0, half), :, pl.ds(c * width, width)], shared[c])

    tiles = 4
    tile = product.shape[0] // tiles

    def multiply(c, start, stop):
        columns = pl.ds(c * width, width)
        right = group[:, :, :, columns].reshape(-1, width)

        @pl.loop(start, stop)
        def _(i):
            rows = pl.ds(pl.multiple_of(i * tile, tile), tile)
            term = contract_cols(base[rows, columns], right)
            product[rows, :] = term if c == 0 else product[rows, :] + term

    def low_start(ref, tokens, name, low, slots):
        loads[name].wait()
        rows = ref[...].reshape(-1, ref.shape[-1])
        low[...] = contract_cols(rows, tokens[...]).astype(bf16)
        return [wires.send(low, slots.at[k - 1], tp_peer(k)) for k in range(1, tps)]

    def low_finish(low, slots, ids):
        total = low[...].astype(f32)
        for k in range(1, tps):
            wires.landed(slots.at[k - 1], ids[k - 1])
            total = total + slots[k - 1].astype(f32)
        return (total * keep_ref[0].astype(f32)).astype(bf16)

    order = far + [0]

    def reduce_start(ref, kept, tokens, x_slots):
        grads = jnp.dot(kept, tokens[...], preferred_element_type=f32).astype(bf16)
        ref[...] = grads.reshape(ref.shape)
        ids = {}
        for k in order:
            for j in range(1, dps):
                ids[j, k] = wires.send(ref.at[dp_of(j), role_of(k)], x_slots.at[j - 1, role_of(k)], dp_peer(j))
        return ids

    def reduce_middle(ref, x_slots, x_ids, s_slots, z_slots, own, steps):
        ids = {}
        for k in steps:
            total = ref[dp, role_of(k)].astype(f32)
            for j in range(1, dps):
                wires.landed(x_slots.at[j - 1, role_of(k)], x_ids[j, k])
                total = total + x_slots[j - 1, role_of(k)].astype(f32)
            if k == 0:
                own[...] = total
            else:
                s_slots[k - 1] = total.astype(bf16)
                ids[k] = wires.send(s_slots.at[k - 1], z_slots.at[k - 1], role_peer(k))
        return ids

    def reduce_finish(own, z_slots, ids):
        total = own[...]
        for k in near:
            wires.landed(z_slots.at[k - 1], ids[k])
            total = total + z_slots[k - 1].astype(f32)
        return total * scale

    def b_copy(i, k):
        block = tp * dps + i
        peer = (role_of(k), block // tps, lax.rem(block, tps))
        place = piece.at[dp, role]
        remote = pltpu.make_async_remote_copy(
            src_ref=b_send.at[i], dst_ref=place, send_sem=b_sends.at[i, k], recv_sem=b_recvs.at[dp, role],
            device_id=peer, device_id_type=MESH,
        )
        if k > 0:
            return None, remote, None
        here = (block // tps == dp) & (lax.rem(block, tps) == tp)
        return here, remote, pltpu.make_async_copy(b_send.at[i], place, b_recvs.at[dp, role])

    def b_start():
        for k in order:
            for i in range(dps):
                here, remote, beside = b_copy(i, k)
                if here is None:
                    remote.start()
                else:
                    pl.when(here)(beside.start)
                    pl.when(jnp.logical_not(here))(remote.start)

    def b_finish():
        for d in range(dps):
            for r in range(roles):
                landed(piece.at[d, r], b_recvs.at[d, r])
        for k in range(roles):
            for i in range(dps):
                here, remote, _ = b_copy(i, k)
                if here is None:
                    remote.wait_send()
                else:
                    pl.when(jnp.logical_not(here))(remote.wait_send)

    b_role, b_dp = gather_start(fb)
    a_home = fa.at[dp, role]
    a_dp = {j: wires.send(a_home, a_home, dp_peer(j)) for j in range(1, dps)}
    a_role = {(0, k): wires.send(a_home, a_home, role_peer(k)) for k in near}
    prompts_near(range(PARTS))
    prompts_across([0])
    gather_forward(fb, b_role, b_dp, near[:1])
    for j in range(1, dps):
        slot = fa.at[dp_back(j), role]
        wires.landed(slot, a_dp[j])
        for k in near:
            a_role[j, k] = wires.send(slot, slot, role_peer(k))
    gather_forward(fb, b_role, b_dp, near[1:])
    loads["base"].start()
    prompts_across([1])
    gather_finish(fb, b_dp)
    b_low = low_start(fb, cot, "cot", lb, rb)
    prompts_across([2])
    for (j, k), place in a_role.items():
        wires.landed(fa.at[dp_back(j), role_back(k)], place)
    a_low = low_start(fa, act, "act", la, ra)
    prompts_across([3])
    prompts_dp_landed([0, 1])

    kept_grad = low_finish(lb, rb, b_low)
    xa_ids = reduce_start(pa, kept_grad, act, xa)
    kept_in = low_finish(la, ra, a_low)
    xb_ids = reduce_start(pb, kept_in, cot, xb)
    prompts_dp_landed([2])
    prompts_hi_landed(range(PARTS))
    prompts_far_landed([0])
    za_ids = reduce_middle(pa, xa, xa_ids, sa, za, oa, order)
    prompts_dp_landed([3])
    loads["own"].wait()
    loads["base"].wait()
    prompts_finish(0)
    multiply(0, 0, 4)
    zb_ids = reduce_middle(pb, xb, xb_ids, sb, zb, ob, order[:2])
    prompts_far_landed([1])

    for name in ("am", "av", "bm", "bv"):
        loads[name].wait()
    fresh, mom, sec = adam_update(a[...], am[...], av[...], reduce_finish(oa, za, za_ids))
    whole[tp, dp, role] = fresh.astype(bf16)
    a_new[...], a_mom[...], a_sec[...] = fresh, mom, sec

    mine = whole.at[tp]
    hi_ids, lo_a = {}, wires.take()

    def onward(j, k):
        slot = mine.at[dp_back(j), role_back(k)]
        for h in range(1, half):
            hi_ids[h, j, k] = wires.send(slot, slot, tp_peer(2 * h))
        wires.send(slot, slot, lo_peer, lo_a)

    def beside(j, k):
        for h in range(1, half):
            slot = whole.at[tp_back(2 * h), dp_back(j), role_back(k)]
            wires.landed(slot, hi_ids[h, j, k])
            wires.send(slot, slot, lo_peer, lo_a)

    a_role, a_dp = gather_start(mine)
    onward(0, 0)
    zb_ids.update(reduce_middle(pb, xb, xb_ids, sb, zb, ob, order[2:]))
    prompts_far_landed([2])
    prompts_finish(1)
    multiply(1, 0, 3)
    gather_forward(mine, a_role, a_dp, near[:1])
    onward(0, near[0])
    multiply(1, 3, 4)
    gather_forward(mine, a_role, a_dp, near[1:2])
    for k in near[1:2]:
        onward(0, k)
    prompts_far_landed([3])
    gather_forward(mine, a_role, a_dp, near[2:])
    for k in near[2:]:
        onward(0, k)

    fresh, mom, sec = adam_update(b[...], bm[...], bv[...], reduce_finish(ob, zb, zb_ids))
    b_new[...], b_mom[...], b_sec[...] = fresh, mom, sec
    columns = fresh.shape[1] // dps
    for i in range(dps):
        b_send[i] = fresh[:, i * columns : (i + 1) * columns].astype(bf16)
    b_start()
    prompts_finish(2)
    for j in range(1, dps):
        for k in [0] + near:
            wires.landed(mine.at[dp_back(j), role_back(k)], a_dp[j, k])
            onward(j, k)
    multiply(2, 0, 4)
    prompts_finish(3)
    for k in [0] + near:
        beside(0, k)
    multiply(3, 0, 4)
    for j in range(1, dps):
        for k in [0] + near:
            beside(j, k)
    wires.landed(whole.at[pl.ds(0, half)], lo_a)
    b_finish()
    wires.drain()
    assert wires.used == recvs.shape[0], wires.used


def step(activations, cotangent, block_keep, a, am, av, b, bm, bv, prompts, base):
    roles, dps, tps = sizes()
    tokens, a_width = activations.shape
    b_width = cotangent.shape[1]
    rows = a.shape[0]
    rank = roles * dps * rows
    bf16, f32 = jnp.bfloat16, jnp.float32
    vmem = pltpu.VMEM
    args = [activations, cotangent, block_keep, a, am, av, b, bm, bv, prompts, base]
    args = [x if x is block_keep else pltpu.with_memory_space_constraint(x, pltpu.HBM) for x in args]
    outs = [vmem(x.shape, f32) for x in (a, a, a, b, b, b)] + [
        vmem((tps, dps, roles, rows, a_width), bf16),
        vmem((dps, roles, rows, b_width // dps), bf16),
        vmem((dps, tps, *prompts.shape), bf16),
        vmem(base.shape, bf16),
        vmem((base.shape[0], dps * tps * prompts.shape[0]), f32),
    ]
    wide = lambda *lead: [vmem((*lead, rows, w), bf16) for w in (a_width, b_width)]
    return pl.pallas_call(
        step_kernel,
        name="step",
        out_shape=outs,
        in_specs=[HBM, HBM, SMEM] + [HBM] * 8,
        out_specs=[VMEM] * len(outs),
        scratch_shapes=[vmem(activations.shape, bf16), vmem(cotangent.shape, bf16)]
        + [vmem(a.shape, f32)] * 3
        + [vmem(b.shape, f32)] * 3
        + wide(dps, roles)
        + [vmem((rank, tokens), bf16)] * 2
        + [vmem((tps - 1, rank, tokens), bf16)] * 2
        + wide(dps, roles)
        + wide(dps - 1, roles)
        + wide(roles - 1)
        + wide(roles - 1)
        + [vmem(a.shape, f32), vmem(b.shape, f32), vmem((dps, rows, b_width // dps), bf16)]
        + [dma(10), dma(1), dma(ARRIVALS), dma(dps, roles), dma(dps, roles)],
        compiler_params=pltpu.CompilerParams(
            collective_id=0, has_side_effects=True, vmem_limit_bytes=16 * 1024 * 1024
        ),
        cost_estimate=pl.CostEstimate(flops=10**9, bytes_accessed=10**7, transcendentals=0),
    )(*args)


def finish_kernel(*refs):
    small, (base, b, a, prompts, product) = refs[:6], refs[6:11]
    copies, (merged_hbm, projected_hbm) = refs[11:17], refs[17:19]
    stage, projected, sems, out_sems, small_sems = refs[19:]
    saves = [pltpu.make_async_copy(x, y, small_sems.at[i]) for i, (x, y) in enumerate(zip(small, copies))]
    for save in saves:
        save.start()
    depth, shards, tile, width = stage.shape
    tiles = base.shape[0] // tile

    def out(i, shard):
        rows = pl.ds(pl.multiple_of(i * tile, tile), tile)
        slot = lax.rem(i, depth)
        target = merged_hbm.at[rows, shard * width : (shard + 1) * width]
        return pltpu.make_async_copy(stage.at[slot, shard], target, sems.at[slot, shard])

    @pl.loop(0, tiles)
    def _(i):
        rows = pl.ds(pl.multiple_of(i * tile, tile), tile)
        left = b[:, rows] * adapter_scale
        for shard in range(shards):

            @pl.when(i >= depth)
            def _():
                out(i - depth, shard).wait()

        for shard in range(shards):
            delta = contract_rows(left, a[shard])
            merged = base[rows, shard * width : (shard + 1) * width].astype(jnp.float32) + delta
            stage[lax.rem(i, depth), shard] = merged.astype(stage.dtype)
            out(i, shard).start()

    low = jnp.zeros((a.shape[1], prompts.shape[0]), jnp.float32)
    for shard in range(shards):
        low = low + contract_cols(a[shard], prompts[:, shard * width : (shard + 1) * width])
    high = low.astype(jnp.bfloat16)
    rest = (low - high.astype(jnp.float32)).astype(jnp.bfloat16)

    saved = []
    for i in range(base.shape[0] // tile):
        rows = pl.ds(i * tile, tile)
        extra = contract_rows(b[:, rows], high) + contract_rows(b[:, rows], rest)
        projected[rows, :] = (product[rows, :] + adapter_scale * extra).astype(projected.dtype)
    last = pltpu.make_async_copy(projected, projected_hbm, out_sems.at[0])
    last.start()

    for i in range(max(tiles - depth, 0), tiles):
        for shard in range(shards):
            out(i, shard).wait()

    for save in saves + [last]:
        save.wait()


def finish(base, b, a, prompts, product, small):
    rows, width = base.shape
    tile = max(t for t in range(128, 257, 128) if rows % t == 0)
    count = prompts.shape[0]
    shards, _, part = a.shape
    vmem = pltpu.VMEM
    args = [pltpu.with_memory_space_constraint(x, pltpu.VMEM) for x in (*small, base, b, a, prompts, product)]
    return pl.pallas_call(
        finish_kernel,
        name="finish",
        out_shape=[pltpu.HBM(x.shape, x.dtype) for x in (*small, base)]
        + [pltpu.HBM((rows, count), jnp.bfloat16)],
        in_specs=[VMEM] * len(args),
        out_specs=[HBM] * (len(small) + 2),
        scratch_shapes=[vmem((2, shards, tile, part), base.dtype), vmem((rows, count), jnp.bfloat16), dma(2, shards), dma(1), dma(len(small))],
        compiler_params=pltpu.CompilerParams(vmem_limit_bytes=16 * 1024 * 1024),
        cost_estimate=pl.CostEstimate(
            flops=2 * rows * width * (count + b.shape[0]), bytes_accessed=4 * rows * width, transcendentals=0
        ),
    )(*args)


def fused_body(
    activations, cotangent, block_keep, input_factor, input_mean, input_square,
    output_factor, output_mean, output_square, frozen_base_rows, prompts,
):
    roles, dps, tps = sizes()
    rank = roles * dps * input_factor.shape[0]
    *small, whole, piece, group, base, product = step(
        activations, cotangent, block_keep, input_factor, input_mean, input_square,
        output_factor, output_mean, output_square, prompts, frozen_base_rows,
    )
    *copies, merged, projected = finish(
        base,
        piece.reshape(rank, -1),
        whole.reshape(tps, rank, -1),
        group.reshape(-1, prompts.shape[1]),
        product,
        small,
    )
    a_new, a_mom, a_sec, b_new, b_mom, b_sec = copies
    return a_new, b_new, a_mom, b_mom, a_sec, b_sec, merged, projected


def chosen_body(*args):
    roles, dps, tps = sizes()
    blocks, rows = args[2].shape[0], args[3].shape[0]
    base_rows = args[9].shape[0]
    fits = rows % 8 == 0 and args[10].shape[0] % 8 == 0 and base_rows % 128 == 0
    if blocks == 1 and min(roles, dps) > 1 and tps % 2 == 0 and fits:
        return fused_body(*args)
    return body(*args)


def solution(mesh):
    placed = (
        P(("role", "dp"), "tp"),
        P(("role", "dp"), "tp"),
        P(("role", "dp")),
        P(("role", "dp"), "tp"),
        P(("role", "dp"), "tp"),
        P(("role", "dp"), "tp"),
        P(("role", "dp"), "tp"),
        P(("role", "dp"), "tp"),
        P(("role", "dp"), "tp"),
        P(("dp", "tp"), None),
        P(("role", "dp", "tp"), None),
    )
    return jax.shard_map(
        chosen_body,
        mesh=mesh,
        in_specs=placed,
        out_specs=(
            P(("role", "dp"), "tp"),
            P(("role", "dp"), "tp"),
            P(("role", "dp"), "tp"),
            P(("role", "dp"), "tp"),
            P(("role", "dp"), "tp"),
            P(("role", "dp"), "tp"),
            P(("dp", "tp"), None),
            P(("dp", "tp"), "role"),
        ),
        check_vma=False,
    )
```

```python
import functools
import math

import jax
import jax.numpy as jnp
from jax import lax
from jax.experimental import pallas as pl
from jax.experimental.pallas import tpu as pltpu
from jax.sharding import PartitionSpec as P

ROLLOUT_TOKENS = 256


adapter_scale = 2.0
learn_rate = 0.004
beta_one = 0.9
beta_two = 0.95
epsilon = 1e-08
first_fix = 1.0 - 0.9**20
second_fix = 1.0 - 0.95**20


def adam_update(factor, moment, square, gradient):
    moment_new = beta_one * moment + (1.0 - beta_one) * gradient
    square_new = beta_two * square + (1.0 - beta_two) * gradient * gradient
    factor_new = factor - learn_rate * (moment_new / first_fix) / (
        jnp.sqrt(square_new / second_fix) + epsilon
    )
    return (factor_new, moment_new, square_new)


def masked(values, block_keep):
    blocks = block_keep.shape[0]
    reshaped_rows = values.reshape(blocks, values.shape[0] // blocks, values.shape[1])
    weighted = reshaped_rows * block_keep.astype(jnp.float32)[:, None, None]
    return weighted.reshape(values.shape).astype(jnp.bfloat16)


def contract_rows(left, right):
    return lax.dot_general(
        left, right, (((0,), (0,)), ((), ())), preferred_element_type=jnp.float32
    )


def contract_cols(left, right):
    return lax.dot_general(
        left, right, (((1,), (1,)), ((), ())), preferred_element_type=jnp.float32
    )


VMEM = pl.BlockSpec(memory_space=pltpu.VMEM)
MESH = pl.DeviceIdType.MESH


def places():
    return tuple(lax.axis_index(name) for name in ("role", "dp", "tp"))


def sizes():
    return tuple(lax.axis_size(name) for name in ("role", "dp", "tp"))


def enter(peers):
    barrier = pltpu.get_barrier_semaphore()
    for peer in peers:
        pl.semaphore_signal(barrier, inc=1, device_id=peer, device_id_type=MESH)
    pl.semaphore_wait(barrier, len(peers))


def send(source, target, send_sem, recv_sem, peer):
    copy = pltpu.make_async_remote_copy(
        src_ref=source,
        dst_ref=target,
        send_sem=send_sem,
        recv_sem=recv_sem,
        device_id=peer,
        device_id_type=MESH,
    )
    copy.start()
    return copy


def landed(slot, sem):
    pltpu.make_async_copy(slot, slot, sem).wait()


def communicate(kernel, name, outs, scratch, collective_id, args):
    return pl.pallas_call(
        kernel,
        name=name,
        out_shape=outs,
        in_specs=[VMEM] * len(args),
        out_specs=[VMEM] * len(outs),
        scratch_shapes=scratch,
        compiler_params=pltpu.CompilerParams(
            collective_id=collective_id,
            has_side_effects=True,
            vmem_limit_bytes=40 * 1024 * 1024,
        ),
        cost_estimate=pl.CostEstimate(
            flops=10**9, bytes_accessed=10**7, transcendentals=0
        ),
    )(*args)


def dma(*shape):
    return pltpu.SemaphoreType.DMA(shape)


def gather_kernel(count, *refs):
    ins, outs = refs[:count], refs[count : 2 * count]
    own, send_role, recv_role, send_dp, recv_dp = refs[2 * count :]
    role, dp, tp = places()
    roles, dps, _ = sizes()
    role_peers = [(lax.rem(role + k, roles), dp, tp) for k in range(1, roles)]
    dp_peers = [(role, lax.rem(dp + j, dps), tp) for j in range(1, dps)]
    enter(role_peers + dp_peers)
    copies = []
    for i in range(count):
        for k in range(1, roles):
            copies.append(send(ins[i], outs[i].at[dp, role], send_role.at[i, k], recv_role.at[i, k], role_peers[k - 1]))
        for j in range(1, dps):
            copies.append(send(ins[i], outs[i].at[dp, role], send_dp.at[i, j, 0], recv_dp.at[i, j, 0], dp_peers[j - 1]))
        local = pltpu.make_async_copy(ins[i], outs[i].at[dp, role], own.at[i])
        local.start()
    for i in range(count):
        for k in range(1, roles):
            slot = outs[i].at[dp, lax.rem(role + roles - k, roles)]
            landed(slot, recv_role.at[i, k])
            for j in range(1, dps):
                copies.append(send(slot, slot, send_dp.at[i, j, k], recv_dp.at[i, j, k], dp_peers[j - 1]))
    for i in range(count):
        pltpu.make_async_copy(ins[i], outs[i].at[dp, role], own.at[i]).wait()
        for j in range(1, dps):
            for k in range(roles):
                slot = outs[i].at[lax.rem(dp + dps - j, dps), lax.rem(role + roles - k, roles)]
                landed(slot, recv_dp.at[i, j, k])
    for copy in copies:
        copy.wait_send()


def gather_rows(arrays):
    roles, dps, _ = sizes()
    n = len(arrays)
    return communicate(
        functools.partial(gather_kernel, n),
        "gather_rows",
        [jax.ShapeDtypeStruct((dps, roles, *x.shape), x.dtype) for x in arrays],
        [dma(n), dma(n, roles), dma(n, roles), dma(n, dps, roles), dma(n, dps, roles)],
        0,
        arrays,
    )


def features_kernel(count, *refs):
    ins, outs = refs[:count], refs[count : 2 * count]
    slots = refs[2 * count : 3 * count]
    sends, recvs = refs[3 * count :]
    role, dp, tp = places()
    tps = sizes()[2]
    peers = [(role, dp, lax.rem(tp + k, tps)) for k in range(1, tps)]
    enter(peers)
    copies = []
    for i in range(count):
        for k in range(1, tps):
            copies.append(send(ins[i], slots[i].at[k - 1], sends.at[i, k], recvs.at[i, k], peers[k - 1]))
    for i in range(count):
        total = ins[i][...]
        for k in range(1, tps):
            landed(slots[i].at[k - 1], recvs.at[i, k])
            total = total + slots[i][k - 1]
        outs[i][...] = total
    for copy in copies:
        copy.wait_send()


def sum_features(arrays):
    tps = sizes()[2]
    n = len(arrays)
    return communicate(
        functools.partial(features_kernel, n),
        "sum_features",
        [jax.ShapeDtypeStruct(x.shape, x.dtype) for x in arrays],
        [pltpu.VMEM((max(tps - 1, 1), *x.shape), x.dtype) for x in arrays] + [dma(n, tps), dma(n, tps)],
        1,
        arrays,
    )


def tokens_kernel(count, *refs):
    ins, outs = refs[:count], refs[count : 2 * count]
    slots = refs[2 * count : 3 * count]
    sends, recvs = refs[3 * count :]
    role, dp, tp = places()
    roles, dps, _ = sizes()
    offsets = [(j, k) for k in range(roles) for j in range(dps) if (j, k) != (0, 0)]
    offsets.sort(key=lambda o: -min(o[1], roles - o[1]))
    peers = {(j, k): (lax.rem(role + k, roles), lax.rem(dp + j, dps), tp) for j, k in offsets}
    enter(list(peers.values()))
    copies = []
    for i in range(count):
        for j, k in offsets:
            peer = peers[j, k]
            copies.append(send(ins[i].at[peer[1], peer[0]], slots[i].at[j, k], sends.at[i, j, k], recvs.at[i, j, k], peer))
    for i in range(count):
        total = ins[i][dp, role].astype(jnp.float32)
        for j, k in reversed(offsets):
            landed(slots[i].at[j, k], recvs.at[i, j, k])
            total = total + slots[i][j, k].astype(jnp.float32)
        outs[i][...] = total
    for copy in copies:
        copy.wait_send()


def sum_tokens(arrays):
    roles, dps, _ = sizes()
    n = len(arrays)
    return communicate(
        functools.partial(tokens_kernel, n),
        "sum_tokens",
        [jax.ShapeDtypeStruct(x.shape[2:], jnp.float32) for x in arrays],
        [pltpu.VMEM(x.shape, x.dtype) for x in arrays] + [dma(n, dps, roles), dma(n, dps, roles)],
        2,
        arrays,
    )


def spread_kernel(a_ref, b_ref, whole_ref, slice_ref, own, send_b, recv_b, send_role, recv_role, send_dp, recv_dp, send_hi, recv_hi, send_lo, recv_lo):
    role, dp, tp = places()
    roles, dps, tps = sizes()
    half = tps // 2
    devices = roles * dps * tps
    me = (role * dps + dp) * tps + tp

    barrier = pltpu.get_barrier_semaphore()

    @pl.loop(1, devices)
    def _(step):
        other = lax.rem(me + step, devices)
        peer = (other // (dps * tps), lax.rem(other // tps, dps), lax.rem(other, tps))
        pl.semaphore_signal(barrier, inc=1, device_id=peer, device_id_type=MESH)

    pl.semaphore_wait(barrier, devices - 1)

    role_peers = [(lax.rem(role + k, roles), dp, tp) for k in range(1, roles)]
    dp_peers = [(role, lax.rem(dp + j, dps), tp) for j in range(1, dps)]
    hi_peers = [(role, dp, lax.rem(tp + 2 * h, tps)) for h in range(1, half)]
    lo_peer = (role, dp, tp + 1 - 2 * lax.rem(tp, 2))

    home = whole_ref.at[tp, dp, role]
    copies = []
    for k in range(1, roles):
        copies.append(send(a_ref, home, send_role.at[k], recv_role.at[k], role_peers[k - 1]))
    for j in range(1, dps):
        copies.append(send(a_ref, home, send_dp.at[j, 0], recv_dp.at[j, 0], dp_peers[j - 1]))
    local = pltpu.make_async_copy(a_ref, home, own.at[0])
    local.start()

    def b_copy(i, k):
        block = tp * dps + i
        peer = (lax.rem(role + k, roles), block // tps, lax.rem(block, tps))
        place = slice_ref.at[dp, role]
        remote = pltpu.make_async_remote_copy(
            src_ref=b_ref.at[i], dst_ref=place, send_sem=send_b.at[i, k], recv_sem=recv_b.at[dp, role],
            device_id=peer, device_id_type=MESH,
        )
        if k > 0:
            return None, remote, None
        here = (block // tps == dp) & (lax.rem(block, tps) == tp)
        return here, remote, pltpu.make_async_copy(b_ref.at[i], place, recv_b.at[dp, role])

    for k in range(roles):
        for i in range(dps):
            here, remote, beside = b_copy(i, k)
            if here is None:
                remote.start()
            else:
                pl.when(here)(beside.start)
                pl.when(jnp.logical_not(here))(remote.start)

    for k in range(1, roles):
        slot = whole_ref.at[tp, dp, lax.rem(role + roles - k, roles)]
        landed(slot, recv_role.at[k])
        for j in range(1, dps):
            copies.append(send(slot, slot, send_dp.at[j, k], recv_dp.at[j, k], dp_peers[j - 1]))
    local.wait()
    for j in range(dps):
        from_dp = lax.rem(dp + dps - j, dps)
        if j > 0:
            for k in range(roles):
                landed(whole_ref.at[tp, from_dp, lax.rem(role + roles - k, roles)], recv_dp.at[j, k])
        group = whole_ref.at[tp, from_dp]
        for h in range(1, half):
            copies.append(send(group, group, send_hi.at[h, j], recv_hi.at[h, j], hi_peers[h - 1]))
        copies.append(send(group, group, send_lo.at[0, j], recv_lo.at[0, j], lo_peer))
    for j in range(dps):
        from_dp = lax.rem(dp + dps - j, dps)
        for h in range(1, half):
            group = whole_ref.at[lax.rem(tp + tps - 2 * h, tps), from_dp]
            landed(group, recv_hi.at[h, j])
            copies.append(send(group, group, send_lo.at[h, j], recv_lo.at[h, j], lo_peer))
    other = lo_peer[2]
    for j in range(dps):
        from_dp = lax.rem(dp + dps - j, dps)
        for h in range(half):
            landed(whole_ref.at[lax.rem(other + tps - 2 * h, tps), from_dp], recv_lo.at[h, j])
    for d in range(dps):
        for r in range(roles):
            landed(slice_ref.at[d, r], recv_b.at[d, r])
    for k in range(roles):
        for i in range(dps):
            here, remote, _ = b_copy(i, k)
            if here is None:
                remote.wait_send()
            else:
                pl.when(jnp.logical_not(here))(remote.wait_send)
    for copy in copies:
        copy.wait_send()


def spread(a, b):
    roles, dps, tps = sizes()
    half = max(tps // 2, 1)
    return communicate(
        spread_kernel,
        "spread",
        [
            jax.ShapeDtypeStruct((tps, dps, roles, *a.shape), a.dtype),
            jax.ShapeDtypeStruct((dps, roles, *b.shape[1:]), b.dtype),
        ],
        [
            dma(1), dma(dps, roles), dma(dps, roles), dma(roles), dma(roles),
            dma(dps, roles), dma(dps, roles), dma(half, dps), dma(half, dps), dma(half, dps), dma(half, dps),
        ],
        3,
        [a, b],
    )


def merge_kernel(base_ref, b_ref, a_ref, prompts_ref, merged_ref, projected_ref):
    shards, _, width = a_ref.shape
    total = jnp.zeros(projected_ref.shape, jnp.float32)
    for shard in range(shards):
        columns = pl.ds(shard * width, width)
        delta = jnp.dot(b_ref[...], a_ref[shard], preferred_element_type=jnp.float32)
        merged = (base_ref[:, columns].astype(jnp.float32) + adapter_scale * delta).astype(jnp.bfloat16)
        merged_ref[:, columns] = merged
        total = total + contract_cols(merged, prompts_ref[:, columns])
    projected_ref[...] = total.astype(projected_ref.dtype)


def merge(base, b, a, prompts):
    rows, width = base.shape
    tile = max(t for t in range(16, 257, 16) if rows % t == 0)
    count = prompts.shape[0]
    return pl.pallas_call(
        merge_kernel,
        name="merge",
        grid=(rows // tile,),
        out_shape=[
            jax.ShapeDtypeStruct(base.shape, base.dtype),
            jax.ShapeDtypeStruct((rows, count), jnp.bfloat16),
        ],
        in_specs=[
            pl.BlockSpec((tile, width), lambda i: (i, 0)),
            pl.BlockSpec((tile, b.shape[1]), lambda i: (i, 0)),
            VMEM,
            VMEM,
        ],
        out_specs=[
            pl.BlockSpec((tile, width), lambda i: (i, 0)),
            pl.BlockSpec((tile, count), lambda i: (i, 0)),
        ],
        compiler_params=pltpu.CompilerParams(vmem_limit_bytes=56 * 1024 * 1024),
        cost_estimate=pl.CostEstimate(
            flops=2 * rows * width * (count + b.shape[1]), bytes_accessed=4 * rows * width, transcendentals=0
        ),
    )(base, b, a, prompts)


def body(
    activations,
    cotangent,
    block_keep,
    input_factor,
    input_mean,
    input_square,
    output_factor,
    output_mean,
    output_square,
    frozen_base_rows,
    prompts,
):
    roles, dps, tps = sizes()
    rows = input_factor.shape[0]
    rank = roles * dps * rows
    group_prompts = lax.all_gather(prompts, ("dp", "tp"), axis=0, tiled=True)
    input_rows, output_rows = gather_rows(
        [input_factor.astype(jnp.bfloat16), output_factor.astype(jnp.bfloat16)]
    )
    low_input = contract_cols(activations, input_rows.reshape(rank, -1))
    low_grad = contract_cols(cotangent, output_rows.reshape(rank, -1))
    low_input, low_grad = sum_features([low_input, low_grad])
    input_kept = masked(low_input, block_keep)
    grad_kept = masked(low_grad, block_keep)
    input_part = contract_rows(grad_kept, activations).astype(jnp.bfloat16)
    output_part = contract_rows(input_kept, cotangent).astype(jnp.bfloat16)
    input_sum, output_sum = sum_tokens(
        [part.reshape(dps, roles, rows, -1) for part in (input_part, output_part)]
    )
    adapter_factor_scale = adapter_scale / ROLLOUT_TOKENS
    input_new, input_moment, input_second = adam_update(
        input_factor, input_mean, input_square, input_sum * adapter_factor_scale
    )
    output_new, output_moment, output_second = adam_update(
        output_factor, output_mean, output_square, output_sum * adapter_factor_scale
    )
    input_send = input_new.astype(jnp.bfloat16)
    output_send = output_new.astype(jnp.bfloat16).reshape(rows, dps, -1).swapaxes(0, 1)
    input_whole, output_slice = spread(input_send, output_send)
    merged_weight_rows, projected = merge(
        frozen_base_rows,
        output_slice.reshape(rank, -1).T,
        input_whole.reshape(tps, rank, -1),
        group_prompts,
    )
    return (
        input_new,
        output_new,
        input_moment,
        output_moment,
        input_second,
        output_second,
        merged_weight_rows,
        projected,
    )


HBM = pl.BlockSpec(memory_space=pltpu.HBM)
SMEM = pl.BlockSpec(memory_space=pltpu.SMEM)
PARTS = 4
ARRIVALS = 66


class Wires:
    def __init__(self, sends, recvs, ruler):
        self.sends, self.recvs, self.ruler, self.used, self.sent = sends, recvs, ruler, 0, 0

    def take(self):
        self.used += 1
        return self.used - 1

    def send(self, source, target, peer, place=None):
        place = self.take() if place is None else place
        send(source, target, self.sends.at[0], self.recvs.at[place], peer)
        self.sent += math.prod(source.shape) * source.dtype.itemsize
        return place

    def landed(self, slot, place):
        landed(slot, self.recvs.at[place])

    def drain(self):
        rows, width = self.ruler.shape
        tiles, rest = divmod(self.sent, 8 * 128 * self.ruler.dtype.itemsize)
        wide = max(w for w in range(1, width // 128 + 1) if tiles % w == 0)
        assert rest == 0 and tiles // wide * 8 <= rows
        landed(self.ruler.at[pl.ds(0, tiles // wide * 8), pl.ds(0, wide * 128)], self.sends.at[0])


def far_first(count):
    return sorted(range(1, count), key=lambda k: -min(k, count - k))


def step_kernel(
    act_hbm, cot_hbm, keep_ref, a_hbm, am_hbm, av_hbm, b_hbm, bm_hbm, bv_hbm, prompts_hbm, base_hbm,
    a_new, a_mom, a_sec, b_new, b_mom, b_sec, whole, piece, group, base, product,
    act, cot, a, am, av, b, bm, bv, fa, fb, la, lb, ra, rb, pa, pb, xa, xb, sa, sb, za, zb, oa, ob, b_send,
    local, sends, recvs, b_sends, b_recvs,
):
    role, dp, tp = places()
    roles, dps, tps = sizes()
    half = tps // 2
    scale = adapter_scale / ROLLOUT_TOKENS
    bf16, f32 = jnp.bfloat16, jnp.float32
    wires = Wires(sends, recvs, base_hbm)

    loads = {}
    pairs = [("a", a_hbm, a), ("b", b_hbm, b), ("act", act_hbm, act), ("cot", cot_hbm, cot), ("am", am_hbm, am),
             ("av", av_hbm, av), ("bm", bm_hbm, bm), ("bv", bv_hbm, bv), ("own", prompts_hbm, group.at[dp, tp])]
    for i, (name, source, target) in enumerate(pairs):
        loads[name] = pltpu.make_async_copy(source, target, local.at[i])
        loads[name].start()
    loads["base"] = pltpu.make_async_copy(base_hbm, base, local.at[len(pairs)])
    loads["base"].start()

    barrier = pltpu.get_barrier_semaphore()
    around = [(lax.rem(role + k, roles), dp, tp) for k in range(1, roles)]
    around += [(role, lax.rem(dp + j, dps), tp) for j in range(1, dps)]
    around += [(role, dp, lax.rem(tp + k, tps)) for k in range(1, tps)]
    for peer in around:
        pl.semaphore_signal(barrier, inc=1, device_id=peer, device_id_type=MESH)

    loads["a"].wait()
    fa[dp, role] = a[...].astype(bf16)
    loads["b"].wait()
    fb[dp, role] = b[...].astype(bf16)
    pl.semaphore_wait(barrier, len(around))

    role_of = lambda k: lax.rem(role + k, roles)
    role_back = lambda k: lax.rem(role + roles - k, roles)
    dp_of = lambda j: lax.rem(dp + j, dps)
    dp_back = lambda j: lax.rem(dp + dps - j, dps)
    tp_back = lambda k: lax.rem(tp + tps - k, tps)
    role_peer = lambda k: (role_of(k), dp, tp)
    dp_peer = lambda j: (role, dp_of(j), tp)
    tp_peer = lambda k: (role, dp, lax.rem(tp + k, tps))
    other = tp + 1 - 2 * lax.rem(tp, 2)
    lo_peer = (role, dp, other)
    far = far_first(roles)
    near = far[::-1]

    def gather_start(ref):
        home = ref.at[dp, role]
        to_role = {k: wires.send(home, home, role_peer(k)) for k in near}
        to_dp = {(j, 0): wires.send(home, home, dp_peer(j)) for j in range(1, dps)}
        return to_role, to_dp

    def gather_forward(ref, to_role, to_dp, steps):
        for k in steps:
            slot = ref.at[dp, role_back(k)]
            wires.landed(slot, to_role[k])
            for j in range(1, dps):
                to_dp[j, k] = wires.send(slot, slot, dp_peer(j))

    def gather_finish(ref, to_dp):
        for (j, k), place in to_dp.items():
            wires.landed(ref.at[dp_back(j), role_back(k)], place)

    width = prompts_hbm.shape[1] // PARTS
    part = lambda ref, c: ref.at[:, pl.ds(c * width, width)]
    spot = lambda d, t, c: group.at[d, t, :, pl.ds(c * width, width)]
    hi_own, dp_own, far_ids = {}, {}, {}
    shared = [wires.take() for _ in range(PARTS)]

    def prompts_near(parts):
        for c in parts:
            for h in range(1, half):
                hi_own[h, c] = wires.send(part(prompts_hbm, c), spot(dp, tp, c), tp_peer(2 * h))
            wires.send(part(prompts_hbm, c), spot(dp, tp, c), lo_peer, shared[c])

    def prompts_across(parts):
        for c in parts:
            for j in range(1, dps):
                dp_own[j, c] = wires.send(part(prompts_hbm, c), spot(dp, tp, c), dp_peer(j))

    def prompts_hi_landed(parts):
        for c in parts:
            for h in range(1, half):
                slot = spot(dp, tp_back(2 * h), c)
                wires.landed(slot, hi_own[h, c])
                wires.send(slot, slot, lo_peer, shared[c])

    def prompts_dp_landed(parts):
        for c in parts:
            for j in range(1, dps):
                slot = spot(dp_back(j), tp, c)
                wires.landed(slot, dp_own[j, c])
                wires.send(slot, slot, lo_peer, shared[c])
                for h in range(1, half):
                    far_ids[j, h, c] = wires.send(slot, slot, tp_peer(2 * h))

    def prompts_far_landed(parts):
        for c in parts:
            for j in range(1, dps):
                for h in range(1, half):
                    slot = spot(dp_back(j), tp_back(2 * h), c)
                    wires.landed(slot, far_ids[j, h, c])
                    wires.send(slot, slot, lo_peer, shared[c])

    def prompts_finish(c):
        wires.landed(group.at[:, pl.ds(0, half), :, pl.ds(c * width, width)], shared[c])

    tiles = 2
    tile = product.shape[0] // tiles

    def multiply(c, start, stop):
        columns = pl.ds(c * width, width)
        right = group[:, :, :, columns].reshape(-1, width)

        @pl.loop(start, stop)
        def _(i):
            rows = pl.ds(pl.multiple_of(i * tile, tile), tile)
            term = contract_cols(base[rows, columns], right)
            product[rows, :] = term if c == 0 else product[rows, :] + term

    def low_start(ref, tokens, name, low, slots):
        loads[name].wait()
        rows = ref[...].reshape(-1, ref.shape[-1])
        low[...] = contract_cols(rows, tokens[...]).astype(bf16)
        return [wires.send(low, slots.at[k - 1], tp_peer(k)) for k in range(1, tps)]

    def low_finish(low, slots, ids):
        total = low[...].astype(f32)
        for k in range(1, tps):
            wires.landed(slots.at[k - 1], ids[k - 1])
            total = total + slots[k - 1].astype(f32)
        return (total * keep_ref[0].astype(f32)).astype(bf16)

    order = far + [0]

    def reduce_start(ref, kept, tokens, x_slots):
        grads = jnp.dot(kept, tokens[...], preferred_element_type=f32).astype(bf16)
        ref[...] = grads.reshape(ref.shape)
        ids = {}
        for k in order:
            for j in range(1, dps):
                ids[j, k] = wires.send(ref.at[dp_of(j), role_of(k)], x_slots.at[j - 1, role_of(k)], dp_peer(j))
        return ids

    def reduce_middle(ref, x_slots, x_ids, s_slots, z_slots, own, steps):
        ids = {}
        for k in steps:
            total = ref[dp, role_of(k)].astype(f32)
            for j in range(1, dps):
                wires.landed(x_slots.at[j - 1, role_of(k)], x_ids[j, k])
                total = total + x_slots[j - 1, role_of(k)].astype(f32)
            if k == 0:
                own[...] = total
            else:
                s_slots[k - 1] = total.astype(bf16)
                ids[k] = wires.send(s_slots.at[k - 1], z_slots.at[k - 1], role_peer(k))
        return ids

    def reduce_finish(own, z_slots, ids):
        total = own[...]
        for k in near:
            wires.landed(z_slots.at[k - 1], ids[k])
            total = total + z_slots[k - 1].astype(f32)
        return total * scale

    def b_copy(i, k):
        block = tp * dps + i
        peer = (role_of(k), block // tps, lax.rem(block, tps))
        place = piece.at[dp, role]
        remote = pltpu.make_async_remote_copy(
            src_ref=b_send.at[i], dst_ref=place, send_sem=b_sends.at[i, k], recv_sem=b_recvs.at[dp, role],
            device_id=peer, device_id_type=MESH,
        )
        if k > 0:
            return None, remote, None
        here = (block // tps == dp) & (lax.rem(block, tps) == tp)
        return here, remote, pltpu.make_async_copy(b_send.at[i], place, b_recvs.at[dp, role])

    def b_start():
        for k in order:
            for i in range(dps):
                here, remote, beside = b_copy(i, k)
                if here is None:
                    remote.start()
                else:
                    pl.when(here)(beside.start)
                    pl.when(jnp.logical_not(here))(remote.start)

    def b_finish():
        for d in range(dps):
            for r in range(roles):
                landed(piece.at[d, r], b_recvs.at[d, r])
        for k in range(roles):
            for i in range(dps):
                here, remote, _ = b_copy(i, k)
                if here is None:
                    remote.wait_send()
                else:
                    pl.when(jnp.logical_not(here))(remote.wait_send)

    b_role, b_dp = gather_start(fb)
    a_home = fa.at[dp, role]
    a_dp = {j: wires.send(a_home, a_home, dp_peer(j)) for j in range(1, dps)}
    a_role = {(0, k): wires.send(a_home, a_home, role_peer(k)) for k in near}
    prompts_near([0, 1, 2])
    prompts_across([0])
    gather_forward(fb, b_role, b_dp, near[:1])
    for j in range(1, dps):
        slot = fa.at[dp_back(j), role]
        wires.landed(slot, a_dp[j])
        for k in near:
            a_role[j, k] = wires.send(slot, slot, role_peer(k))
    gather_forward(fb, b_role, b_dp, near[1:])
    prompts_dp_landed([0])
    prompts_across([1])
    gather_finish(fb, b_dp)
    b_low = low_start(fb, cot, "cot", lb, rb)
    prompts_across([2])
    for (j, k), place in a_role.items():
        wires.landed(fa.at[dp_back(j), role_back(k)], place)
    a_low = low_start(fa, act, "act", la, ra)
    prompts_across([3])
    prompts_hi_landed([0, 1, 2])
    prompts_far_landed([0])
    prompts_dp_landed([1])
    prompts_near([3])
    loads["own"].wait()
    loads["base"].wait()
    prompts_finish(0)
    multiply(0, 0, 2)

    kept_grad = low_finish(lb, rb, b_low)
    xa_ids = reduce_start(pa, kept_grad, act, xa)
    kept_in = low_finish(la, ra, a_low)
    xb_ids = reduce_start(pb, kept_in, cot, xb)
    prompts_dp_landed([2])
    prompts_far_landed([1])
    za_ids = reduce_middle(pa, xa, xa_ids, sa, za, oa, order)
    prompts_dp_landed([3])
    prompts_finish(1)
    multiply(1, 0, 2)
    zb_ids = reduce_middle(pb, xb, xb_ids, sb, zb, ob, order[:2])
    prompts_hi_landed([3])

    for name in ("am", "av", "bm", "bv"):
        loads[name].wait()
    fresh, mom, sec = adam_update(a[...], am[...], av[...], reduce_finish(oa, za, za_ids))
    whole[tp, dp, role] = fresh.astype(bf16)
    a_new[...], a_mom[...], a_sec[...] = fresh, mom, sec

    mine = whole.at[tp]
    hi_ids, lo_a = {}, wires.take()

    y_first = [0] + near[: roles // 2 - 1]
    late_dp = {}

    def onward(j, k):
        slot = mine.at[dp_back(j), role_back(k)]
        if j == 0 or k not in y_first:
            for h in range(1, half):
                hi_ids[h, j, k] = wires.send(slot, slot, tp_peer(2 * h))
        wires.send(slot, slot, lo_peer, lo_a)

    def beside(j, k):
        for h in range(1, half):
            slot = whole.at[tp_back(2 * h), dp_back(j), role_back(k)]
            wires.landed(slot, late_dp[h, j, k] if j > 0 and k in y_first else hi_ids[h, j, k])
            if j == 0 and k in y_first:
                for other_j in range(1, dps):
                    late_dp[h, other_j, k] = wires.send(slot, slot, dp_peer(other_j))
            wires.send(slot, slot, lo_peer, lo_a)

    a_role, a_dp = gather_start(mine)
    onward(0, 0)
    zb_ids.update(reduce_middle(pb, xb, xb_ids, sb, zb, ob, order[2:]))
    prompts_far_landed([2])
    prompts_finish(2)
    multiply(2, 0, 2)
    gather_forward(mine, a_role, a_dp, near[:1])
    onward(0, near[0])
    gather_forward(mine, a_role, a_dp, near[1:2])
    for k in near[1:2]:
        onward(0, k)
    prompts_far_landed([3])
    gather_forward(mine, a_role, a_dp, near[2:])
    for k in near[2:]:
        onward(0, k)

    fresh, mom, sec = adam_update(b[...], bm[...], bv[...], reduce_finish(ob, zb, zb_ids))
    b_new[...], b_mom[...], b_sec[...] = fresh, mom, sec
    columns = fresh.shape[1] // dps
    for i in range(dps):
        b_send[i] = fresh[:, i * columns : (i + 1) * columns].astype(bf16)
    b_start()
    prompts_finish(3)
    y_last = [k for k in near if k not in y_first]
    for k in y_first + y_last:
        if k in y_first:
            beside(0, k)
        for j in range(1, dps):
            wires.landed(mine.at[dp_back(j), role_back(k)], a_dp[j, k])
            onward(j, k)
    multiply(3, 0, 2)
    for k in y_last:
        beside(0, k)
    for k in y_first + y_last:
        for j in range(1, dps):
            beside(j, k)
    wires.landed(whole.at[pl.ds(0, half)], lo_a)
    b_finish()
    wires.drain()
    assert wires.used == recvs.shape[0], wires.used


def step(activations, cotangent, block_keep, a, am, av, b, bm, bv, prompts, base):
    roles, dps, tps = sizes()
    tokens, a_width = activations.shape
    b_width = cotangent.shape[1]
    rows = a.shape[0]
    rank = roles * dps * rows
    bf16, f32 = jnp.bfloat16, jnp.float32
    vmem = pltpu.VMEM
    args = [activations, cotangent, block_keep, a, am, av, b, bm, bv, prompts, base]
    args = [x if x is block_keep else pltpu.with_memory_space_constraint(x, pltpu.HBM) for x in args]
    outs = [vmem(x.shape, f32) for x in (a, a, a, b, b, b)] + [
        vmem((tps, dps, roles, rows, a_width), bf16),
        vmem((dps, roles, rows, b_width // dps), bf16),
        vmem((dps, tps, *prompts.shape), bf16),
        vmem(base.shape, bf16),
        vmem((base.shape[0], dps * tps * prompts.shape[0]), f32),
    ]
    wide = lambda *lead: [vmem((*lead, rows, w), bf16) for w in (a_width, b_width)]
    return pl.pallas_call(
        step_kernel,
        name="step",
        out_shape=outs,
        in_specs=[HBM, HBM, SMEM] + [HBM] * 8,
        out_specs=[VMEM] * len(outs),
        scratch_shapes=[vmem(activations.shape, bf16), vmem(cotangent.shape, bf16)]
        + [vmem(a.shape, f32)] * 3
        + [vmem(b.shape, f32)] * 3
        + wide(dps, roles)
        + [vmem((rank, tokens), bf16)] * 2
        + [vmem((tps - 1, rank, tokens), bf16)] * 2
        + wide(dps, roles)
        + wide(dps - 1, roles)
        + wide(roles - 1)
        + wide(roles - 1)
        + [vmem(a.shape, f32), vmem(b.shape, f32), vmem((dps, rows, b_width // dps), bf16)]
        + [dma(10), dma(1), dma(ARRIVALS), dma(dps, roles), dma(dps, roles)],
        compiler_params=pltpu.CompilerParams(
            collective_id=0, has_side_effects=True, vmem_limit_bytes=16 * 1024 * 1024
        ),
        cost_estimate=pl.CostEstimate(flops=10**9, bytes_accessed=10**7, transcendentals=0),
    )(*args)


def finish_kernel(*refs):
    small, (base, b, a, prompts, product) = refs[:6], refs[6:11]
    copies, (merged_hbm, projected_hbm) = refs[11:17], refs[17:19]
    stage, projected, sems, out_sems, small_sems = refs[19:]
    saves = [pltpu.make_async_copy(x, y, small_sems.at[i]) for i, (x, y) in enumerate(zip(small, copies))]
    for save in saves:
        save.start()
    depth, shards, groups, eight, width = stage.shape
    tile = groups * eight
    tiles = base.shape[0] // groups

    def out(i, shard):
        rows = pl.ds(i * groups, groups)
        slot = lax.rem(i, depth)
        target = merged_hbm.at[rows, :, shard * width : (shard + 1) * width]
        return pltpu.make_async_copy(stage.at[slot, shard], target, sems.at[slot, shard])

    @pl.loop(0, tiles)
    def _(i):
        rows = pl.ds(i * groups, groups)
        left = b[:, pl.ds(pl.multiple_of(i * tile, tile), tile)] * adapter_scale
        for shard in range(shards):

            @pl.when(i >= depth)
            def _():
                out(i - depth, shard).wait()

        for shard in range(shards):
            delta = contract_rows(left, a[shard]).reshape(groups, eight, width)
            merged = base[rows, :, shard * width : (shard + 1) * width].astype(jnp.float32) + delta
            stage[lax.rem(i, depth), shard] = merged.astype(stage.dtype)
            out(i, shard).start()

    low = jnp.zeros((a.shape[1], prompts.shape[0]), jnp.float32)
    for shard in range(shards):
        low = low + contract_cols(a[shard], prompts[:, shard * width : (shard + 1) * width])
    high = low.astype(jnp.bfloat16)
    rest = (low - high.astype(jnp.float32)).astype(jnp.bfloat16)

    saved = []
    for i in range(tiles):
        rows = pl.ds(i * tile, tile)
        extra = contract_rows(b[:, rows], high) + contract_rows(b[:, rows], rest)
        projected[rows, :] = (product[rows, :] + adapter_scale * extra).astype(projected.dtype)
    last = pltpu.make_async_copy(projected, projected_hbm, out_sems.at[0])
    last.start()

    for i in range(max(tiles - depth, 0), tiles):
        for shard in range(shards):
            out(i, shard).wait()

    for save in saves + [last]:
        save.wait()


def finish(base, b, a, prompts, product, small):
    rows, width = base.shape
    tile = max(t for t in range(128, 257, 128) if rows % t == 0)
    count = prompts.shape[0]
    shards, _, part = a.shape
    vmem = pltpu.VMEM
    base = base.reshape(rows // 8, 8, width)
    args = [pltpu.with_memory_space_constraint(x, pltpu.VMEM) for x in (*small, base, b, a, prompts, product)]
    return pl.pallas_call(
        finish_kernel,
        name="finish",
        out_shape=[pltpu.HBM(x.shape, x.dtype) for x in (*small, base)]
        + [pltpu.HBM((rows, count), jnp.bfloat16)],
        in_specs=[VMEM] * len(args),
        out_specs=[HBM] * (len(small) + 2),
        scratch_shapes=[vmem((2, shards, tile // 8, 8, part), base.dtype), vmem((rows, count), jnp.bfloat16), dma(2, shards), dma(1), dma(len(small))],
        compiler_params=pltpu.CompilerParams(vmem_limit_bytes=16 * 1024 * 1024),
        cost_estimate=pl.CostEstimate(
            flops=2 * rows * width * (count + b.shape[0]), bytes_accessed=4 * rows * width, transcendentals=0
        ),
    )(*args)


def fused_body(
    activations, cotangent, block_keep, input_factor, input_mean, input_square,
    output_factor, output_mean, output_square, frozen_base_rows, prompts,
):
    roles, dps, tps = sizes()
    rank = roles * dps * input_factor.shape[0]
    *small, whole, piece, group, base, product = step(
        activations, cotangent, block_keep, input_factor, input_mean, input_square,
        output_factor, output_mean, output_square, prompts, frozen_base_rows,
    )
    *copies, merged, projected = finish(
        base,
        piece.reshape(rank, -1),
        whole.reshape(tps, rank, -1),
        group.reshape(-1, prompts.shape[1]),
        product,
        small,
    )
    a_new, a_mom, a_sec, b_new, b_mom, b_sec = copies
    merged = merged.reshape(frozen_base_rows.shape)
    return a_new, b_new, a_mom, b_mom, a_sec, b_sec, merged, projected


def chosen_body(*args):
    roles, dps, tps = sizes()
    blocks, rows = args[2].shape[0], args[3].shape[0]
    base_rows = args[9].shape[0]
    fits = rows % 8 == 0 and args[10].shape[0] % 8 == 0 and base_rows % 128 == 0
    if blocks == 1 and min(roles, dps) > 1 and tps % 2 == 0 and fits:
        return fused_body(*args)
    return body(*args)


def solution(mesh):
    placed = (
        P(("role", "dp"), "tp"),
        P(("role", "dp"), "tp"),
        P(("role", "dp")),
        P(("role", "dp"), "tp"),
        P(("role", "dp"), "tp"),
        P(("role", "dp"), "tp"),
        P(("role", "dp"), "tp"),
        P(("role", "dp"), "tp"),
        P(("role", "dp"), "tp"),
        P(("dp", "tp"), None),
        P(("role", "dp", "tp"), None),
    )
    return jax.shard_map(
        chosen_body,
        mesh=mesh,
        in_specs=placed,
        out_specs=(
            P(("role", "dp"), "tp"),
            P(("role", "dp"), "tp"),
            P(("role", "dp"), "tp"),
            P(("role", "dp"), "tp"),
            P(("role", "dp"), "tp"),
            P(("role", "dp"), "tp"),
            P(("dp", "tp"), None),
            P(("dp", "tp"), "role"),
        ),
        check_vma=False,
    )
```

```python
import functools
import math

import jax
import jax.numpy as jnp
from jax import lax
from jax.experimental import pallas as pl
from jax.experimental.pallas import tpu as pltpu
from jax.sharding import PartitionSpec as P

ROLLOUT_TOKENS = 256


adapter_scale = 2.0
learn_rate = 0.004
beta_one = 0.9
beta_two = 0.95
epsilon = 1e-08
first_fix = 1.0 - 0.9**20
second_fix = 1.0 - 0.95**20


def adam_update(factor, moment, square, gradient):
    moment_new = beta_one * moment + (1.0 - beta_one) * gradient
    square_new = beta_two * square + (1.0 - beta_two) * gradient * gradient
    factor_new = factor - learn_rate * (moment_new / first_fix) / (
        jnp.sqrt(square_new / second_fix) + epsilon
    )
    return (factor_new, moment_new, square_new)


def masked(values, block_keep):
    blocks = block_keep.shape[0]
    reshaped_rows = values.reshape(blocks, values.shape[0] // blocks, values.shape[1])
    weighted = reshaped_rows * block_keep.astype(jnp.float32)[:, None, None]
    return weighted.reshape(values.shape).astype(jnp.bfloat16)


def contract_rows(left, right):
    return lax.dot_general(
        left, right, (((0,), (0,)), ((), ())), preferred_element_type=jnp.float32
    )


def contract_cols(left, right):
    return lax.dot_general(
        left, right, (((1,), (1,)), ((), ())), preferred_element_type=jnp.float32
    )


VMEM = pl.BlockSpec(memory_space=pltpu.VMEM)
MESH = pl.DeviceIdType.MESH


def places():
    return tuple(lax.axis_index(name) for name in ("role", "dp", "tp"))


def sizes():
    return tuple(lax.axis_size(name) for name in ("role", "dp", "tp"))


def enter(peers):
    barrier = pltpu.get_barrier_semaphore()
    for peer in peers:
        pl.semaphore_signal(barrier, inc=1, device_id=peer, device_id_type=MESH)
    pl.semaphore_wait(barrier, len(peers))


def send(source, target, send_sem, recv_sem, peer):
    copy = pltpu.make_async_remote_copy(
        src_ref=source,
        dst_ref=target,
        send_sem=send_sem,
        recv_sem=recv_sem,
        device_id=peer,
        device_id_type=MESH,
    )
    copy.start()
    return copy


def landed(slot, sem):
    pltpu.make_async_copy(slot, slot, sem).wait()


def communicate(kernel, name, outs, scratch, collective_id, args):
    return pl.pallas_call(
        kernel,
        name=name,
        out_shape=outs,
        in_specs=[VMEM] * len(args),
        out_specs=[VMEM] * len(outs),
        scratch_shapes=scratch,
        compiler_params=pltpu.CompilerParams(
            collective_id=collective_id,
            has_side_effects=True,
            vmem_limit_bytes=40 * 1024 * 1024,
        ),
        cost_estimate=pl.CostEstimate(
            flops=10**9, bytes_accessed=10**7, transcendentals=0
        ),
    )(*args)


def dma(*shape):
    return pltpu.SemaphoreType.DMA(shape)


def gather_kernel(count, *refs):
    ins, outs = refs[:count], refs[count : 2 * count]
    own, send_role, recv_role, send_dp, recv_dp = refs[2 * count :]
    role, dp, tp = places()
    roles, dps, _ = sizes()
    role_peers = [(lax.rem(role + k, roles), dp, tp) for k in range(1, roles)]
    dp_peers = [(role, lax.rem(dp + j, dps), tp) for j in range(1, dps)]
    enter(role_peers + dp_peers)
    copies = []
    for i in range(count):
        for k in range(1, roles):
            copies.append(send(ins[i], outs[i].at[dp, role], send_role.at[i, k], recv_role.at[i, k], role_peers[k - 1]))
        for j in range(1, dps):
            copies.append(send(ins[i], outs[i].at[dp, role], send_dp.at[i, j, 0], recv_dp.at[i, j, 0], dp_peers[j - 1]))
        local = pltpu.make_async_copy(ins[i], outs[i].at[dp, role], own.at[i])
        local.start()
    for i in range(count):
        for k in range(1, roles):
            slot = outs[i].at[dp, lax.rem(role + roles - k, roles)]
            landed(slot, recv_role.at[i, k])
            for j in range(1, dps):
                copies.append(send(slot, slot, send_dp.at[i, j, k], recv_dp.at[i, j, k], dp_peers[j - 1]))
    for i in range(count):
        pltpu.make_async_copy(ins[i], outs[i].at[dp, role], own.at[i]).wait()
        for j in range(1, dps):
            for k in range(roles):
                slot = outs[i].at[lax.rem(dp + dps - j, dps), lax.rem(role + roles - k, roles)]
                landed(slot, recv_dp.at[i, j, k])
    for copy in copies:
        copy.wait_send()


def gather_rows(arrays):
    roles, dps, _ = sizes()
    n = len(arrays)
    return communicate(
        functools.partial(gather_kernel, n),
        "gather_rows",
        [jax.ShapeDtypeStruct((dps, roles, *x.shape), x.dtype) for x in arrays],
        [dma(n), dma(n, roles), dma(n, roles), dma(n, dps, roles), dma(n, dps, roles)],
        0,
        arrays,
    )


def features_kernel(count, *refs):
    ins, outs = refs[:count], refs[count : 2 * count]
    slots = refs[2 * count : 3 * count]
    sends, recvs = refs[3 * count :]
    role, dp, tp = places()
    tps = sizes()[2]
    peers = [(role, dp, lax.rem(tp + k, tps)) for k in range(1, tps)]
    enter(peers)
    copies = []
    for i in range(count):
        for k in range(1, tps):
            copies.append(send(ins[i], slots[i].at[k - 1], sends.at[i, k], recvs.at[i, k], peers[k - 1]))
    for i in range(count):
        total = ins[i][...]
        for k in range(1, tps):
            landed(slots[i].at[k - 1], recvs.at[i, k])
            total = total + slots[i][k - 1]
        outs[i][...] = total
    for copy in copies:
        copy.wait_send()


def sum_features(arrays):
    tps = sizes()[2]
    n = len(arrays)
    return communicate(
        functools.partial(features_kernel, n),
        "sum_features",
        [jax.ShapeDtypeStruct(x.shape, x.dtype) for x in arrays],
        [pltpu.VMEM((max(tps - 1, 1), *x.shape), x.dtype) for x in arrays] + [dma(n, tps), dma(n, tps)],
        1,
        arrays,
    )


def tokens_kernel(count, *refs):
    ins, outs = refs[:count], refs[count : 2 * count]
    slots = refs[2 * count : 3 * count]
    sends, recvs = refs[3 * count :]
    role, dp, tp = places()
    roles, dps, _ = sizes()
    offsets = [(j, k) for k in range(roles) for j in range(dps) if (j, k) != (0, 0)]
    offsets.sort(key=lambda o: -min(o[1], roles - o[1]))
    peers = {(j, k): (lax.rem(role + k, roles), lax.rem(dp + j, dps), tp) for j, k in offsets}
    enter(list(peers.values()))
    copies = []
    for i in range(count):
        for j, k in offsets:
            peer = peers[j, k]
            copies.append(send(ins[i].at[peer[1], peer[0]], slots[i].at[j, k], sends.at[i, j, k], recvs.at[i, j, k], peer))
    for i in range(count):
        total = ins[i][dp, role].astype(jnp.float32)
        for j, k in reversed(offsets):
            landed(slots[i].at[j, k], recvs.at[i, j, k])
            total = total + slots[i][j, k].astype(jnp.float32)
        outs[i][...] = total
    for copy in copies:
        copy.wait_send()


def sum_tokens(arrays):
    roles, dps, _ = sizes()
    n = len(arrays)
    return communicate(
        functools.partial(tokens_kernel, n),
        "sum_tokens",
        [jax.ShapeDtypeStruct(x.shape[2:], jnp.float32) for x in arrays],
        [pltpu.VMEM(x.shape, x.dtype) for x in arrays] + [dma(n, dps, roles), dma(n, dps, roles)],
        2,
        arrays,
    )


def spread_kernel(a_ref, b_ref, whole_ref, slice_ref, own, send_b, recv_b, send_role, recv_role, send_dp, recv_dp, send_hi, recv_hi, send_lo, recv_lo):
    role, dp, tp = places()
    roles, dps, tps = sizes()
    half = tps // 2
    devices = roles * dps * tps
    me = (role * dps + dp) * tps + tp

    barrier = pltpu.get_barrier_semaphore()

    @pl.loop(1, devices)
    def _(step):
        other = lax.rem(me + step, devices)
        peer = (other // (dps * tps), lax.rem(other // tps, dps), lax.rem(other, tps))
        pl.semaphore_signal(barrier, inc=1, device_id=peer, device_id_type=MESH)

    pl.semaphore_wait(barrier, devices - 1)

    role_peers = [(lax.rem(role + k, roles), dp, tp) for k in range(1, roles)]
    dp_peers = [(role, lax.rem(dp + j, dps), tp) for j in range(1, dps)]
    hi_peers = [(role, dp, lax.rem(tp + 2 * h, tps)) for h in range(1, half)]
    lo_peer = (role, dp, tp + 1 - 2 * lax.rem(tp, 2))

    home = whole_ref.at[tp, dp, role]
    copies = []
    for k in range(1, roles):
        copies.append(send(a_ref, home, send_role.at[k], recv_role.at[k], role_peers[k - 1]))
    for j in range(1, dps):
        copies.append(send(a_ref, home, send_dp.at[j, 0], recv_dp.at[j, 0], dp_peers[j - 1]))
    local = pltpu.make_async_copy(a_ref, home, own.at[0])
    local.start()

    def b_copy(i, k):
        block = tp * dps + i
        peer = (lax.rem(role + k, roles), block // tps, lax.rem(block, tps))
        place = slice_ref.at[dp, role]
        remote = pltpu.make_async_remote_copy(
            src_ref=b_ref.at[i], dst_ref=place, send_sem=send_b.at[i, k], recv_sem=recv_b.at[dp, role],
            device_id=peer, device_id_type=MESH,
        )
        if k > 0:
            return None, remote, None
        here = (block // tps == dp) & (lax.rem(block, tps) == tp)
        return here, remote, pltpu.make_async_copy(b_ref.at[i], place, recv_b.at[dp, role])

    for k in range(roles):
        for i in range(dps):
            here, remote, beside = b_copy(i, k)
            if here is None:
                remote.start()
            else:
                pl.when(here)(beside.start)
                pl.when(jnp.logical_not(here))(remote.start)

    for k in range(1, roles):
        slot = whole_ref.at[tp, dp, lax.rem(role + roles - k, roles)]
        landed(slot, recv_role.at[k])
        for j in range(1, dps):
            copies.append(send(slot, slot, send_dp.at[j, k], recv_dp.at[j, k], dp_peers[j - 1]))
    local.wait()
    for j in range(dps):
        from_dp = lax.rem(dp + dps - j, dps)
        if j > 0:
            for k in range(roles):
                landed(whole_ref.at[tp, from_dp, lax.rem(role + roles - k, roles)], recv_dp.at[j, k])
        group = whole_ref.at[tp, from_dp]
        for h in range(1, half):
            copies.append(send(group, group, send_hi.at[h, j], recv_hi.at[h, j], hi_peers[h - 1]))
        copies.append(send(group, group, send_lo.at[0, j], recv_lo.at[0, j], lo_peer))
    for j in range(dps):
        from_dp = lax.rem(dp + dps - j, dps)
        for h in range(1, half):
            group = whole_ref.at[lax.rem(tp + tps - 2 * h, tps), from_dp]
            landed(group, recv_hi.at[h, j])
            copies.append(send(group, group, send_lo.at[h, j], recv_lo.at[h, j], lo_peer))
    other = lo_peer[2]
    for j in range(dps):
        from_dp = lax.rem(dp + dps - j, dps)
        for h in range(half):
            landed(whole_ref.at[lax.rem(other + tps - 2 * h, tps), from_dp], recv_lo.at[h, j])
    for d in range(dps):
        for r in range(roles):
            landed(slice_ref.at[d, r], recv_b.at[d, r])
    for k in range(roles):
        for i in range(dps):
            here, remote, _ = b_copy(i, k)
            if here is None:
                remote.wait_send()
            else:
                pl.when(jnp.logical_not(here))(remote.wait_send)
    for copy in copies:
        copy.wait_send()


def spread(a, b):
    roles, dps, tps = sizes()
    half = max(tps // 2, 1)
    return communicate(
        spread_kernel,
        "spread",
        [
            jax.ShapeDtypeStruct((tps, dps, roles, *a.shape), a.dtype),
            jax.ShapeDtypeStruct((dps, roles, *b.shape[1:]), b.dtype),
        ],
        [
            dma(1), dma(dps, roles), dma(dps, roles), dma(roles), dma(roles),
            dma(dps, roles), dma(dps, roles), dma(half, dps), dma(half, dps), dma(half, dps), dma(half, dps),
        ],
        3,
        [a, b],
    )


def merge_kernel(base_ref, b_ref, a_ref, prompts_ref, merged_ref, projected_ref):
    shards, _, width = a_ref.shape
    total = jnp.zeros(projected_ref.shape, jnp.float32)
    for shard in range(shards):
        columns = pl.ds(shard * width, width)
        delta = jnp.dot(b_ref[...], a_ref[shard], preferred_element_type=jnp.float32)
        merged = (base_ref[:, columns].astype(jnp.float32) + adapter_scale * delta).astype(jnp.bfloat16)
        merged_ref[:, columns] = merged
        total = total + contract_cols(merged, prompts_ref[:, columns])
    projected_ref[...] = total.astype(projected_ref.dtype)


def merge(base, b, a, prompts):
    rows, width = base.shape
    tile = max(t for t in range(16, 257, 16) if rows % t == 0)
    count = prompts.shape[0]
    return pl.pallas_call(
        merge_kernel,
        name="merge",
        grid=(rows // tile,),
        out_shape=[
            jax.ShapeDtypeStruct(base.shape, base.dtype),
            jax.ShapeDtypeStruct((rows, count), jnp.bfloat16),
        ],
        in_specs=[
            pl.BlockSpec((tile, width), lambda i: (i, 0)),
            pl.BlockSpec((tile, b.shape[1]), lambda i: (i, 0)),
            VMEM,
            VMEM,
        ],
        out_specs=[
            pl.BlockSpec((tile, width), lambda i: (i, 0)),
            pl.BlockSpec((tile, count), lambda i: (i, 0)),
        ],
        compiler_params=pltpu.CompilerParams(vmem_limit_bytes=56 * 1024 * 1024),
        cost_estimate=pl.CostEstimate(
            flops=2 * rows * width * (count + b.shape[1]), bytes_accessed=4 * rows * width, transcendentals=0
        ),
    )(base, b, a, prompts)


def body(
    activations,
    cotangent,
    block_keep,
    input_factor,
    input_mean,
    input_square,
    output_factor,
    output_mean,
    output_square,
    frozen_base_rows,
    prompts,
):
    roles, dps, tps = sizes()
    rows = input_factor.shape[0]
    rank = roles * dps * rows
    group_prompts = lax.all_gather(prompts, ("dp", "tp"), axis=0, tiled=True)
    input_rows, output_rows = gather_rows(
        [input_factor.astype(jnp.bfloat16), output_factor.astype(jnp.bfloat16)]
    )
    low_input = contract_cols(activations, input_rows.reshape(rank, -1))
    low_grad = contract_cols(cotangent, output_rows.reshape(rank, -1))
    low_input, low_grad = sum_features([low_input, low_grad])
    input_kept = masked(low_input, block_keep)
    grad_kept = masked(low_grad, block_keep)
    input_part = contract_rows(grad_kept, activations).astype(jnp.bfloat16)
    output_part = contract_rows(input_kept, cotangent).astype(jnp.bfloat16)
    input_sum, output_sum = sum_tokens(
        [part.reshape(dps, roles, rows, -1) for part in (input_part, output_part)]
    )
    adapter_factor_scale = adapter_scale / ROLLOUT_TOKENS
    input_new, input_moment, input_second = adam_update(
        input_factor, input_mean, input_square, input_sum * adapter_factor_scale
    )
    output_new, output_moment, output_second = adam_update(
        output_factor, output_mean, output_square, output_sum * adapter_factor_scale
    )
    input_send = input_new.astype(jnp.bfloat16)
    output_send = output_new.astype(jnp.bfloat16).reshape(rows, dps, -1).swapaxes(0, 1)
    input_whole, output_slice = spread(input_send, output_send)
    merged_weight_rows, projected = merge(
        frozen_base_rows,
        output_slice.reshape(rank, -1).T,
        input_whole.reshape(tps, rank, -1),
        group_prompts,
    )
    return (
        input_new,
        output_new,
        input_moment,
        output_moment,
        input_second,
        output_second,
        merged_weight_rows,
        projected,
    )


HBM = pl.BlockSpec(memory_space=pltpu.HBM)
SMEM = pl.BlockSpec(memory_space=pltpu.SMEM)
PARTS = 4
ARRIVALS = 66


class Wires:
    def __init__(self, sends, recvs, ruler):
        self.sends, self.recvs, self.ruler, self.used, self.sent = sends, recvs, ruler, 0, 0

    def take(self):
        self.used += 1
        return self.used - 1

    def send(self, source, target, peer, place=None):
        place = self.take() if place is None else place
        send(source, target, self.sends.at[0], self.recvs.at[place], peer)
        self.sent += math.prod(source.shape) * source.dtype.itemsize
        return place

    def landed(self, slot, place):
        landed(slot, self.recvs.at[place])

    def drain(self):
        rows, width = self.ruler.shape
        tiles, rest = divmod(self.sent, 8 * 128 * self.ruler.dtype.itemsize)
        wide = max(w for w in range(1, width // 128 + 1) if tiles % w == 0)
        assert rest == 0 and tiles // wide * 8 <= rows
        landed(self.ruler.at[pl.ds(0, tiles // wide * 8), pl.ds(0, wide * 128)], self.sends.at[0])


def far_first(count):
    return sorted(range(1, count), key=lambda k: -min(k, count - k))


def step_kernel(
    act_hbm, cot_hbm, keep_ref, a_hbm, am_hbm, av_hbm, b_hbm, bm_hbm, bv_hbm, prompts_hbm, base_hbm,
    a_new, a_mom, a_sec, b_new, b_mom, b_sec, whole, piece, group, base, product,
    act, cot, a, am, av, b, bm, bv, fa, fb, la, lb, ra, rb, pa, pb, xa, xb, sa, sb, za, zb, oa, ob, b_send,
    local, sends, recvs, b_sends, b_recvs,
):
    role, dp, tp = places()
    roles, dps, tps = sizes()
    half = tps // 2
    scale = adapter_scale / ROLLOUT_TOKENS
    bf16, f32 = jnp.bfloat16, jnp.float32
    wires = Wires(sends, recvs, base_hbm)

    loads = {}
    pairs = [("a", a_hbm, a), ("b", b_hbm, b), ("act", act_hbm, act), ("cot", cot_hbm, cot), ("am", am_hbm, am),
             ("av", av_hbm, av), ("bm", bm_hbm, bm), ("bv", bv_hbm, bv), ("own", prompts_hbm, group.at[dp, tp])]
    for i, (name, source, target) in enumerate(pairs):
        loads[name] = pltpu.make_async_copy(source, target, local.at[i])
        loads[name].start()
    loads["base"] = pltpu.make_async_copy(base_hbm, base, local.at[len(pairs)])
    loads["base"].start()

    barrier = pltpu.get_barrier_semaphore()
    around = [(lax.rem(role + k, roles), dp, tp) for k in range(1, roles)]
    around += [(role, lax.rem(dp + j, dps), tp) for j in range(1, dps)]
    around += [(role, dp, lax.rem(tp + k, tps)) for k in range(1, tps)]
    for peer in around:
        pl.semaphore_signal(barrier, inc=1, device_id=peer, device_id_type=MESH)

    loads["a"].wait()
    fa[dp, role] = a[...].astype(bf16)
    loads["b"].wait()
    fb[dp, role] = b[...].astype(bf16)
    pl.semaphore_wait(barrier, len(around))

    role_of = lambda k: lax.rem(role + k, roles)
    role_back = lambda k: lax.rem(role + roles - k, roles)
    dp_of = lambda j: lax.rem(dp + j, dps)
    dp_back = lambda j: lax.rem(dp + dps - j, dps)
    tp_back = lambda k: lax.rem(tp + tps - k, tps)
    role_peer = lambda k: (role_of(k), dp, tp)
    dp_peer = lambda j: (role, dp_of(j), tp)
    tp_peer = lambda k: (role, dp, lax.rem(tp + k, tps))
    other = tp + 1 - 2 * lax.rem(tp, 2)
    lo_peer = (role, dp, other)
    far = far_first(roles)
    near = far[::-1]

    def gather_start(ref):
        home = ref.at[dp, role]
        to_role = {k: wires.send(home, home, role_peer(k)) for k in near}
        to_dp = {(j, 0): wires.send(home, home, dp_peer(j)) for j in range(1, dps)}
        return to_role, to_dp

    def gather_forward(ref, to_role, to_dp, steps):
        for k in steps:
            slot = ref.at[dp, role_back(k)]
            wires.landed(slot, to_role[k])
            for j in range(1, dps):
                to_dp[j, k] = wires.send(slot, slot, dp_peer(j))

    def gather_finish(ref, to_dp):
        for (j, k), place in to_dp.items():
            wires.landed(ref.at[dp_back(j), role_back(k)], place)

    width = prompts_hbm.shape[1] // PARTS
    part = lambda ref, c: ref.at[:, pl.ds(c * width, width)]
    spot = lambda d, t, c: group.at[d, t, :, pl.ds(c * width, width)]
    hi_own, dp_own, far_ids = {}, {}, {}
    shared = [wires.take() for _ in range(PARTS)]

    def prompts_near(parts):
        for c in parts:
            for h in range(1, half):
                hi_own[h, c] = wires.send(part(prompts_hbm, c), spot(dp, tp, c), tp_peer(2 * h))
            wires.send(part(prompts_hbm, c), spot(dp, tp, c), lo_peer, shared[c])

    def prompts_across(parts):
        for c in parts:
            for j in range(1, dps):
                dp_own[j, c] = wires.send(part(prompts_hbm, c), spot(dp, tp, c), dp_peer(j))

    def prompts_hi_landed(parts):
        for c in parts:
            for h in range(1, half):
                slot = spot(dp, tp_back(2 * h), c)
                wires.landed(slot, hi_own[h, c])
                wires.send(slot, slot, lo_peer, shared[c])

    def prompts_dp_landed(parts):
        for c in parts:
            for j in range(1, dps):
                slot = spot(dp_back(j), tp, c)
                wires.landed(slot, dp_own[j, c])
                wires.send(slot, slot, lo_peer, shared[c])
                for h in range(1, half):
                    far_ids[j, h, c] = wires.send(slot, slot, tp_peer(2 * h))

    def prompts_far_landed(parts):
        for c in parts:
            for j in range(1, dps):
                for h in range(1, half):
                    slot = spot(dp_back(j), tp_back(2 * h), c)
                    wires.landed(slot, far_ids[j, h, c])
                    wires.send(slot, slot, lo_peer, shared[c])

    def prompts_finish(c):
        wires.landed(group.at[:, pl.ds(0, half), :, pl.ds(c * width, width)], shared[c])

    tiles = 2
    tile = product.shape[0] // tiles

    def multiply(c, start, stop):
        columns = pl.ds(c * width, width)
        right = group[:, :, :, columns].reshape(-1, width)

        @pl.loop(start, stop)
        def _(i):
            rows = pl.ds(pl.multiple_of(i * tile, tile), tile)
            term = contract_cols(base[rows, columns], right)
            product[rows, :] = term if c == 0 else product[rows, :] + term

    def low_start(ref, tokens, name, low, slots):
        loads[name].wait()
        rows = ref[...].reshape(-1, ref.shape[-1])
        low[...] = contract_cols(rows, tokens[...]).astype(bf16)
        return [wires.send(low, slots.at[k - 1], tp_peer(k)) for k in range(1, tps)]

    def low_finish(low, slots, ids):
        total = low[...].astype(f32)
        for k in range(1, tps):
            wires.landed(slots.at[k - 1], ids[k - 1])
            total = total + slots[k - 1].astype(f32)
        return (total * keep_ref[0].astype(f32)).astype(bf16)

    order = far + [0]

    def reduce_start(ref, kept, tokens, x_slots):
        grads = jnp.dot(kept, tokens[...], preferred_element_type=f32).astype(bf16)
        ref[...] = grads.reshape(ref.shape)
        ids = {}
        for k in order:
            for j in range(1, dps):
                ids[j, k] = wires.send(ref.at[dp_of(j), role_of(k)], x_slots.at[j - 1, role_of(k)], dp_peer(j))
        return ids

    def reduce_middle(ref, x_slots, x_ids, s_slots, z_slots, own, steps):
        ids = {}
        for k in steps:
            total = ref[dp, role_of(k)].astype(f32)
            for j in range(1, dps):
                wires.landed(x_slots.at[j - 1, role_of(k)], x_ids[j, k])
                total = total + x_slots[j - 1, role_of(k)].astype(f32)
            if k == 0:
                own[...] = total
            else:
                s_slots[k - 1] = total.astype(bf16)
                ids[k] = wires.send(s_slots.at[k - 1], z_slots.at[k - 1], role_peer(k))
        return ids

    def reduce_finish(own, z_slots, ids):
        total = own[...]
        for k in near:
            wires.landed(z_slots.at[k - 1], ids[k])
            total = total + z_slots[k - 1].astype(f32)
        return total * scale

    def b_copy(i, k):
        block = tp * dps + i
        peer = (role_of(k), block // tps, lax.rem(block, tps))
        place = piece.at[dp, role]
        remote = pltpu.make_async_remote_copy(
            src_ref=b_send.at[i], dst_ref=place, send_sem=b_sends.at[i, k], recv_sem=b_recvs.at[dp, role],
            device_id=peer, device_id_type=MESH,
        )
        if k > 0:
            return None, remote, None
        here = (block // tps == dp) & (lax.rem(block, tps) == tp)
        return here, remote, pltpu.make_async_copy(b_send.at[i], place, b_recvs.at[dp, role])

    def b_start():
        for k in order:
            for i in range(dps):
                here, remote, beside = b_copy(i, k)
                if here is None:
                    remote.start()
                else:
                    pl.when(here)(beside.start)
                    pl.when(jnp.logical_not(here))(remote.start)

    def b_finish():
        for d in range(dps):
            for r in range(roles):
                landed(piece.at[d, r], b_recvs.at[d, r])
        for k in range(roles):
            for i in range(dps):
                here, remote, _ = b_copy(i, k)
                if here is None:
                    remote.wait_send()
                else:
                    pl.when(jnp.logical_not(here))(remote.wait_send)

    b_role, b_dp = gather_start(fb)
    a_home = fa.at[dp, role]
    a_dp = {j: wires.send(a_home, a_home, dp_peer(j)) for j in range(1, dps)}
    a_role = {(0, k): wires.send(a_home, a_home, role_peer(k)) for k in near}
    prompts_near([0, 1, 2])
    prompts_across([0])
    gather_forward(fb, b_role, b_dp, near[:1])
    for j in range(1, dps):
        slot = fa.at[dp_back(j), role]
        wires.landed(slot, a_dp[j])
        for k in near:
            a_role[j, k] = wires.send(slot, slot, role_peer(k))
    gather_forward(fb, b_role, b_dp, near[1:])
    prompts_dp_landed([0])
    prompts_across([1])
    gather_finish(fb, b_dp)
    b_low = low_start(fb, cot, "cot", lb, rb)
    prompts_across([2])
    for (j, k), place in a_role.items():
        wires.landed(fa.at[dp_back(j), role_back(k)], place)
    a_low = low_start(fa, act, "act", la, ra)
    prompts_across([3])
    prompts_hi_landed([0, 1, 2])
    prompts_far_landed([0])
    prompts_dp_landed([1])
    prompts_near([3])

    kept_grad = low_finish(lb, rb, b_low)
    xa_ids = reduce_start(pa, kept_grad, act, xa)
    kept_in = low_finish(la, ra, a_low)
    xb_ids = reduce_start(pb, kept_in, cot, xb)
    prompts_dp_landed([2])
    prompts_far_landed([1])
    za_ids = reduce_middle(pa, xa, xa_ids, sa, za, oa, order)
    prompts_dp_landed([3])
    loads["own"].wait()
    loads["base"].wait()
    prompts_finish(0)
    multiply(0, 0, 2)
    zb_ids = reduce_middle(pb, xb, xb_ids, sb, zb, ob, order[:1])
    prompts_hi_landed([3])
    prompts_far_landed([2])

    for name in ("am", "av", "bm", "bv"):
        loads[name].wait()
    fresh, mom, sec = adam_update(a[...], am[...], av[...], reduce_finish(oa, za, za_ids))
    whole[tp, dp, role] = fresh.astype(bf16)
    a_new[...], a_mom[...], a_sec[...] = fresh, mom, sec

    mine = whole.at[tp]
    hi_ids, lo_a = {}, wires.take()

    y_first = [0] + near[: roles // 2 - 1]
    late_dp = {}

    def onward(j, k):
        slot = mine.at[dp_back(j), role_back(k)]
        if j == 0 or k not in y_first:
            for h in range(1, half):
                hi_ids[h, j, k] = wires.send(slot, slot, tp_peer(2 * h))
        wires.send(slot, slot, lo_peer, lo_a)

    def beside(j, k):
        for h in range(1, half):
            slot = whole.at[tp_back(2 * h), dp_back(j), role_back(k)]
            wires.landed(slot, late_dp[h, j, k] if j > 0 and k in y_first else hi_ids[h, j, k])
            if j == 0 and k in y_first:
                for other_j in range(1, dps):
                    late_dp[h, other_j, k] = wires.send(slot, slot, dp_peer(other_j))
            wires.send(slot, slot, lo_peer, lo_a)

    a_role, a_dp = gather_start(mine)
    onward(0, 0)
    zb_ids.update(reduce_middle(pb, xb, xb_ids, sb, zb, ob, order[1:]))
    prompts_finish(1)
    multiply(1, 0, 2)
    gather_forward(mine, a_role, a_dp, near[:1])
    onward(0, near[0])
    gather_forward(mine, a_role, a_dp, near[1:2])
    for k in near[1:2]:
        onward(0, k)
    prompts_far_landed([3])
    gather_forward(mine, a_role, a_dp, near[2:])
    for k in near[2:]:
        onward(0, k)

    fresh, mom, sec = adam_update(b[...], bm[...], bv[...], reduce_finish(ob, zb, zb_ids))
    b_new[...], b_mom[...], b_sec[...] = fresh, mom, sec
    columns = fresh.shape[1] // dps
    for i in range(dps):
        b_send[i] = fresh[:, i * columns : (i + 1) * columns].astype(bf16)
    b_start()
    prompts_finish(2)
    multiply(2, 0, 2)
    y_last = [k for k in near if k not in y_first]
    for k in y_first + y_last:
        if k in y_first:
            beside(0, k)
        for j in range(1, dps):
            wires.landed(mine.at[dp_back(j), role_back(k)], a_dp[j, k])
            onward(j, k)
    prompts_finish(3)
    multiply(3, 0, 2)
    for k in y_last:
        beside(0, k)
    for k in y_first + y_last:
        for j in range(1, dps):
            beside(j, k)
    wires.landed(whole.at[pl.ds(0, half)], lo_a)
    b_finish()
    wires.drain()
    assert wires.used == recvs.shape[0], wires.used


def step(activations, cotangent, block_keep, a, am, av, b, bm, bv, prompts, base):
    roles, dps, tps = sizes()
    tokens, a_width = activations.shape
    b_width = cotangent.shape[1]
    rows = a.shape[0]
    rank = roles * dps * rows
    bf16, f32 = jnp.bfloat16, jnp.float32
    vmem = pltpu.VMEM
    args = [activations, cotangent, block_keep, a, am, av, b, bm, bv, prompts, base]
    args = [x if x is block_keep else pltpu.with_memory_space_constraint(x, pltpu.HBM) for x in args]
    outs = [vmem(x.shape, f32) for x in (a, a, a, b, b, b)] + [
        vmem((tps, dps, roles, rows, a_width), bf16),
        vmem((dps, roles, rows, b_width // dps), bf16),
        vmem((dps, tps, *prompts.shape), bf16),
        vmem(base.shape, bf16),
        vmem((base.shape[0], dps * tps * prompts.shape[0]), f32),
    ]
    wide = lambda *lead: [vmem((*lead, rows, w), bf16) for w in (a_width, b_width)]
    return pl.pallas_call(
        step_kernel,
        name="step",
        out_shape=outs,
        in_specs=[HBM, HBM, SMEM] + [HBM] * 8,
        out_specs=[VMEM] * len(outs),
        scratch_shapes=[vmem(activations.shape, bf16), vmem(cotangent.shape, bf16)]
        + [vmem(a.shape, f32)] * 3
        + [vmem(b.shape, f32)] * 3
        + wide(dps, roles)
        + [vmem((rank, tokens), bf16)] * 2
        + [vmem((tps - 1, rank, tokens), bf16)] * 2
        + wide(dps, roles)
        + wide(dps - 1, roles)
        + wide(roles - 1)
        + wide(roles - 1)
        + [vmem(a.shape, f32), vmem(b.shape, f32), vmem((dps, rows, b_width // dps), bf16)]
        + [dma(10), dma(1), dma(ARRIVALS), dma(dps, roles), dma(dps, roles)],
        compiler_params=pltpu.CompilerParams(
            collective_id=0, has_side_effects=True, vmem_limit_bytes=16 * 1024 * 1024
        ),
        cost_estimate=pl.CostEstimate(flops=10**9, bytes_accessed=10**7, transcendentals=0),
    )(*args)


def finish_kernel(*refs):
    small, (base, b, a, prompts, product) = refs[:6], refs[6:11]
    copies, (merged_hbm, projected_hbm) = refs[11:17], refs[17:19]
    stage, projected, sems, out_sems, small_sems = refs[19:]
    saves = [pltpu.make_async_copy(x, y, small_sems.at[i]) for i, (x, y) in enumerate(zip(small, copies))]
    for save in saves:
        save.start()
    depth, shards, groups, eight, width = stage.shape
    tile = groups * eight
    tiles = base.shape[0] // groups

    def out(i, shard):
        rows = pl.ds(i * groups, groups)
        slot = lax.rem(i, depth)
        target = merged_hbm.at[rows, :, shard * width : (shard + 1) * width]
        return pltpu.make_async_copy(stage.at[slot, shard], target, sems.at[slot, shard])

    @pl.loop(0, tiles)
    def _(i):
        rows = pl.ds(i * groups, groups)
        left = b[:, pl.ds(pl.multiple_of(i * tile, tile), tile)] * adapter_scale
        for shard in range(shards):

            @pl.when(i >= depth)
            def _():
                out(i - depth, shard).wait()

        for shard in range(shards):
            delta = contract_rows(left, a[shard]).reshape(groups, eight, width)
            merged = base[rows, :, shard * width : (shard + 1) * width].astype(jnp.float32) + delta
            stage[lax.rem(i, depth), shard] = merged.astype(stage.dtype)
            out(i, shard).start()

    low = jnp.zeros((a.shape[1], prompts.shape[0]), jnp.float32)
    for shard in range(shards):
        low = low + contract_cols(a[shard], prompts[:, shard * width : (shard + 1) * width])
    high = low.astype(jnp.bfloat16)
    rest = (low - high.astype(jnp.float32)).astype(jnp.bfloat16)

    saved = []
    for i in range(tiles):
        rows = pl.ds(i * tile, tile)
        extra = contract_rows(b[:, rows], high) + contract_rows(b[:, rows], rest)
        projected[rows, :] = (product[rows, :] + adapter_scale * extra).astype(projected.dtype)
    last = pltpu.make_async_copy(projected, projected_hbm, out_sems.at[0])
    last.start()

    for i in range(max(tiles - depth, 0), tiles):
        for shard in range(shards):
            out(i, shard).wait()

    for save in saves + [last]:
        save.wait()


def finish(base, b, a, prompts, product, small):
    rows, width = base.shape
    tile = max(t for t in range(128, 257, 128) if rows % t == 0)
    count = prompts.shape[0]
    shards, _, part = a.shape
    vmem = pltpu.VMEM
    base = base.reshape(rows // 8, 8, width)
    args = [pltpu.with_memory_space_constraint(x, pltpu.VMEM) for x in (*small, base, b, a, prompts, product)]
    return pl.pallas_call(
        finish_kernel,
        name="finish",
        out_shape=[pltpu.HBM(x.shape, x.dtype) for x in (*small, base)]
        + [pltpu.HBM((rows, count), jnp.bfloat16)],
        in_specs=[VMEM] * len(args),
        out_specs=[HBM] * (len(small) + 2),
        scratch_shapes=[vmem((2, shards, tile // 8, 8, part), base.dtype), vmem((rows, count), jnp.bfloat16), dma(2, shards), dma(1), dma(len(small))],
        compiler_params=pltpu.CompilerParams(vmem_limit_bytes=16 * 1024 * 1024),
        cost_estimate=pl.CostEstimate(
            flops=2 * rows * width * (count + b.shape[0]), bytes_accessed=4 * rows * width, transcendentals=0
        ),
    )(*args)


def fused_body(
    activations, cotangent, block_keep, input_factor, input_mean, input_square,
    output_factor, output_mean, output_square, frozen_base_rows, prompts,
):
    roles, dps, tps = sizes()
    rank = roles * dps * input_factor.shape[0]
    *small, whole, piece, group, base, product = step(
        activations, cotangent, block_keep, input_factor, input_mean, input_square,
        output_factor, output_mean, output_square, prompts, frozen_base_rows,
    )
    *copies, merged, projected = finish(
        base,
        piece.reshape(rank, -1),
        whole.reshape(tps, rank, -1),
        group.reshape(-1, prompts.shape[1]),
        product,
        small,
    )
    a_new, a_mom, a_sec, b_new, b_mom, b_sec = copies
    merged = merged.reshape(frozen_base_rows.shape)
    return a_new, b_new, a_mom, b_mom, a_sec, b_sec, merged, projected


def chosen_body(*args):
    roles, dps, tps = sizes()
    blocks, rows = args[2].shape[0], args[3].shape[0]
    base_rows = args[9].shape[0]
    fits = rows % 8 == 0 and args[10].shape[0] % 8 == 0 and base_rows % 128 == 0
    if blocks == 1 and min(roles, dps) > 1 and tps % 2 == 0 and fits:
        return fused_body(*args)
    return body(*args)


def solution(mesh):
    placed = (
        P(("role", "dp"), "tp"),
        P(("role", "dp"), "tp"),
        P(("role", "dp")),
        P(("role", "dp"), "tp"),
        P(("role", "dp"), "tp"),
        P(("role", "dp"), "tp"),
        P(("role", "dp"), "tp"),
        P(("role", "dp"), "tp"),
        P(("role", "dp"), "tp"),
        P(("dp", "tp"), None),
        P(("role", "dp", "tp"), None),
    )
    return jax.shard_map(
        chosen_body,
        mesh=mesh,
        in_specs=placed,
        out_specs=(
            P(("role", "dp"), "tp"),
            P(("role", "dp"), "tp"),
            P(("role", "dp"), "tp"),
            P(("role", "dp"), "tp"),
            P(("role", "dp"), "tp"),
            P(("role", "dp"), "tp"),
            P(("dp", "tp"), None),
            P(("dp", "tp"), "role"),
        ),
        check_vma=False,
    )
```
